32 devices in a mesh: dp: 1 (over z), tp: 32 (over y, x, core).
Axes of the slice: x: 4, y: 4, z: 1, core: 2. Of those that a mesh axis runs over, the one named last changes fastest.
The devices are a block of a 4x4x8 slice.
Arguments:
- ids: int32 [2, 256], P('dp')
- emb: bfloat16 [65536, 3584], P('tp')
- g: bfloat16 [3584], replicated
- w: bfloat16 [3584, 8192], P(None, 'tp')
- du: bfloat16 [2, 256, 8192], P('dp', None, 'tp')
- dres: bfloat16 [2, 256, 3584], P('dp', 'tp')
Outputs:
- output 1: bfloat16 [2, 256, 8192], P('dp', None, 'tp')
- output 2: bfloat16 [2, 256, 3584], P('dp', 'tp')
- output 3: float32 [65536, 3584], P(('dp', 'tp'))
- output 4: float32 [3584, 8192], P(None, ('dp', 'tp'))
- output 5: float32 [3584], P('dp')
All inputs are finite; a program needn't handle non-finite values.
Results may differ from the reference program's by a relative error of at most 0.001.
Values are sent between devices in bfloat16 or wider.
A program may use at most 768 MiB of HBM per device.

```python
import jax
import jax.numpy as jnp
from jax import lax

K = 2
T = 256
V = 65536
D = 3584
FC = 8192
GROUP = 32
EPS = 1e-6
NPOOL = K * T // 16
FCG = FC // GROUP


def setup_inputs(seed: int = 0, part: int = 0) -> dict:
    key = jax.random.key(seed)
    kp = jax.random.fold_in(key, part)
    ke, kg, kw = jax.random.split(key, 3)
    k1, k2, k3, k4, k5, k6 = jax.random.split(kp, 6)
    ka, kb, kc = jax.random.split(jax.random.fold_in(kp, 7), 3)
    a = jax.random.randint(ka, (K, T), 0, V)
    b = jax.random.randint(kb, (K, T), 0, V)
    coin = jax.random.bernoulli(kc, 0.4, (K, T))
    ids = jnp.where(coin, a, jnp.minimum(a, b)).astype(jnp.int32)
    emb = jax.random.normal(ke, (V, D), jnp.float32).astype(jnp.bfloat16)
    g = (1.0 + 0.5 * jax.random.normal(kg, (D,), jnp.float32)).astype(jnp.bfloat16)
    w = (jax.random.normal(kw, (D, FC), jnp.float32) * D ** -0.5).astype(jnp.bfloat16)
    du = (jax.random.normal(k5, (K, T, FC), jnp.float32) * (D / FC) ** 0.5).astype(jnp.bfloat16)
    dres = jax.random.normal(k6, (K, T, D), jnp.float32).astype(jnp.bfloat16)
    return {"ids": ids, "emb": emb, "g": g, "w": w, "du": du, "dres": dres}


def reference(ids, emb, g, w, du, dres):
    gf = g.astype(jnp.float32)

    def micro(carry, inp):
        de, dw, dg = carry
        idm, dum, drm = inp
        x = emb[idm]
        xf = x.astype(jnp.float32)
        rs = lax.rsqrt(jnp.mean(xf * xf, axis=-1, keepdims=True) + EPS)
        nh = xf * rs
        n = (nh * gf).astype(jnp.bfloat16)
        u = jnp.dot(n, w, preferred_element_type=jnp.float32).astype(jnp.bfloat16)
        dn = jnp.zeros((T, D), jnp.float32)
        for j in range(GROUP):
            pb = jnp.dot(dum[:, j * FCG:(j + 1) * FCG], w[:, j * FCG:(j + 1) * FCG].T, preferred_element_type=jnp.float32)
            dn = dn + pb.astype(jnp.bfloat16).astype(jnp.float32)
        gdn = gf * dn
        dxn = rs * (gdn - nh * jnp.mean(nh * gdn, axis=-1, keepdims=True))
        dx = (drm.astype(jnp.float32) + dxn).astype(jnp.bfloat16)
        de = de.at[idm].add(dx.astype(jnp.float32))
        dw = dw + jnp.dot(n.T, dum, preferred_element_type=jnp.float32)
        dg = dg + jnp.sum(dn * nh, axis=0)
        return (de, dw, dg), (u, x)

    init = (jnp.zeros((V, D), jnp.float32), jnp.zeros((D, FC), jnp.float32), jnp.zeros((D,), jnp.float32))
    (de, dw, dg), (u, x) = lax.scan(micro, init, (ids, du, dres))
    return u, x, de, dw, dg
```

```python
import functools
import math

import jax
import jax.numpy as jnp
from jax import lax
from jax.experimental import pallas as pl
from jax.experimental.pallas import tpu as pltpu
from jax.sharding import PartitionSpec as P

EPS = 1e-6
F32 = jnp.float32
BF16 = jnp.bfloat16
VMEM = pltpu.VMEM
DMA = pltpu.SemaphoreType.DMA


def comm_kernel(dims, loc_ref, emb_ref, g_ref, w_ref, du_ref, dres_ref,
                x_ref, nall_ref, dxall_ref, dg_ref,
                ebuf, esem, dup, oh, pdn, rpdn, s1, r1, t1, r2, xp, rxp, rx1, tx, rx2,
                own, gn, gd, dgp, dgs, dgx, dgy,
                pair_s, pair_r, rs_s, rs_r, ag_s, ag_r, sib_s, sib_r, dg_s, dg_r, osem):
    k, tl, d, n = dims["k"], dims["tl"], dims["d"], dims["n"]
    dh, dq, cw = d // 2, d // 4, dims["cw"]
    nch = dh // cw
    tb = k * tl
    me = lax.axis_index("tp")
    c = lax.rem(me, 2)
    x = lax.rem(me // 2, n)
    y = me // (2 * n)

    def dev(yy, xx, cc):
        return {"tp": (yy * n + xx) * 2 + cc}

    def add(v, s):
        return lax.rem(v + s + n, n)

    coord = {"x": x, "y": y}

    def peer(axis, s):
        return dev(y, add(x, s), c) if axis == "x" else dev(add(y, s), x, c)

    sib = dev(y, x, 1 - c)
    sends = []

    def remote(src, dst, ss, rs, to):
        cp = pltpu.make_async_remote_copy(src_ref=src, dst_ref=dst, send_sem=ss, recv_sem=rs,
                                          device_id=to, device_id_type=pl.DeviceIdType.MESH)
        cp.start()
        sends.append(cp)
        return cp

    barrier = pltpu.get_barrier_semaphore()
    greet = [sib] + [peer(a, s) for a in ("x", "y") for s in (1, -1, 2)]
    for to in greet:
        pl.semaphore_signal(barrier, inc=1, device_id=to, device_id_type=pl.DeviceIdType.MESH)

    eload = []
    for h in range(2):
        cp = pltpu.make_async_copy(emb_ref.at[:, pl.ds(h * dh, dh)], ebuf.at[h], esem.at[h])
        cp.start()
        eload.append(cp)

    duf = [du_ref[m].astype(F32) for m in range(k)]
    for cc in range(2):
        for b in range(n * n):
            r = b * 2 + cc
            blk = jnp.concatenate([v[r * tl:(r + 1) * tl] for v in duf], axis=0)
            dup[pl.ds((cc * n * n + b) * tb, tb), :] = blk.astype(BF16)

    def scatter_rows(dst, h, j, val):
        cols = pl.ds(pl.multiple_of(j * cw, cw), cw)
        for cc in range(2):
            for yy in range(n):
                for xx in range(n):
                    p, q = (xx, yy) if h == 0 else (yy, xx)
                    row = ((cc * n + yy) * n + xx) * tb
                    dst[h, cc, p, pl.ds(q * tb, tb), cols] = val[row:row + tb]

    pair = []
    for h in range(2):
        @pl.loop(0, nch)
        def _(j):
            wj = w_ref[pl.ds(pl.multiple_of(h * dh + j * cw, cw), cw), :]
            v = lax.dot_general(dup[...], wj, (((1,), (1,)), ((), ())), preferred_element_type=F32)
            scatter_rows(pdn, h, j, v.astype(BF16))

        if h == 0:
            pl.semaphore_wait(barrier, len(greet))
        pair.append(remote(pdn.at[h, 1 - c], rpdn.at[h], pair_s.at[0, h], pair_r.at[0, h], sib))

    ids = lax.broadcasted_iota(jnp.int32, (tb * n, oh.shape[1]), 1)
    for i in range(2 * n):
        rows = pl.ds(i * tb * n, tb * n)
        oh[rows, :] = (loc_ref[rows, :] == ids).astype(BF16)

    class Ring:
        def __init__(self, sem, axis, s, r):
            self.sem, self.axis, self.s, self.r = sem, axis, s, r
            self.p = coord[axis]

        def half(self, sgn):
            return pl.ds(0 if sgn > 0 else dq, dq)

        def send(self, msg, sgn, block, half):
            i = 0 if sgn > 0 else 1
            st, h, ph = self.sem
            return remote(self.s.at[block, :, half], self.r.at[msg, i],
                          rs_s.at[st, h, ph, msg, i], rs_r.at[st, h, ph, msg, i], peer(self.axis, sgn))

        def start(self):
            self.a1 = [self.send(0, sg, add(self.p, 2), self.half(sg)) for sg in (1, -1)]
            self.a2 = [self.send(1, sg, add(self.p, sg), self.half(-sg)) for sg in (1, -1)]

        def mid(self):
            self.b = []
            for i, sg in enumerate((1, -1)):
                self.a1[i].wait_recv()
                blk, hf = add(self.p, sg), self.half(sg)
                self.s[blk, :, hf] = self.s[blk, :, hf] + self.r[0, i]
                self.b.append(self.send(2, sg, blk, hf))

        def finish(self):
            for cp in self.a2 + self.b:
                cp.wait_recv()
            for i, sg in enumerate((1, -1)):
                hf = self.half(sg)
                yield hf, self.s[self.p, :, hf] + self.r[2, i] + self.r[1, 1 - i]

    axes = [("x", "y"), ("y", "x")]

    def first(st, h, s, r):
        return Ring((st, h, 0), axes[h][0], s, r.at[h])

    def second(st, h, t, r):
        return Ring((st, h, 1), axes[h][1], t.at[h], r.at[h])

    d1 = [first(0, h, s1.at[h], r1) for h in range(2)]
    d2 = [second(0, h, t1, r2) for h in range(2)]
    x1 = [first(1, h, xp.at[h, c], rx1) for h in range(2)]
    x2 = [second(1, h, tx, rx2) for h in range(2)]

    def finish1(ring, t, h):
        for hf, v in ring.finish():
            t[h, :, :, hf] = v.reshape(n, tb, dq)

    for h in range(2):
        pair[h].wait_recv()
        for p in range(n):
            s1[h, p] = pdn[h, c, p].astype(F32) + rpdn[h, p].astype(F32)
        d1[h].start()

    xpair = []
    for h in range(2):
        eload[h].wait()

        @pl.loop(0, nch)
        def _(j):
            ej = ebuf[h, :, pl.ds(pl.multiple_of(j * cw, cw), cw)]
            v = jnp.dot(oh[...], ej, preferred_element_type=F32)
            scatter_rows(xp, h, j, v.astype(BF16))

        xpair.append(remote(xp.at[h, 1 - c], rxp.at[h], pair_s.at[1, h], pair_r.at[1, h], sib))
        if h == 0:
            for hh in range(2):
                d1[hh].mid()

    for h in range(2):
        xpair[h].wait_recv()
        for p in range(n):
            xp[h, c, p] = xp[h, c, p] + rxp[h, p]
        x1[h].start()
    for h in range(2):
        finish1(d1[h], t1, h)
        d2[h].start()
    for h in range(2):
        x1[h].mid()
    for h in range(2):
        d2[h].mid()
    for h in range(2):
        finish1(x1[h], tx, h)
        x2[h].start()
    for h in range(2):
        x2[h].mid()

    class Gather:
        def __init__(self, sem, axis, get):
            self.sem, self.axis, self.get = sem, axis, get
            self.p = coord[axis]

        def send(self, msg, sgn, block, half):
            i = 0 if sgn > 0 else 1
            st, h, ph = self.sem
            ref = self.get(block, half)
            return remote(ref, ref, ag_s.at[st, h, ph, msg, i], ag_r.at[st, h, ph, msg, i],
                          peer(self.axis, sgn))

        def start(self):
            self.a = [self.send(0, sg, self.p, pl.ds(0, dh)) for sg in (1, -1)]

        def mid(self):
            self.b = []
            for i, sg in enumerate((1, -1)):
                self.a[i].wait_recv()
                self.b.append(self.send(1, sg, add(self.p, -sg), pl.ds(0 if sg > 0 else dq, dq)))

        def finish(self):
            for cp in self.b:
                cp.wait_recv()

    def gathers(st, g):
        ph1, ph2 = [], []
        ph1.append(Gather((st, 0, 0), "x", lambda i, hf: g.at[0, c, y, i, :, hf]))
        ph2.append(Gather((st, 0, 1), "y", lambda i, hf: g.at[0, c, i, :, :, hf]))
        ph1.append(Gather((st, 1, 0), "y", lambda i, hf: g.at[1, c, i, x, :, hf]))
        ph2.append(Gather((st, 1, 1), "x", lambda i, hf: g.at[1, c, :, i, :, hf]))
        return ph1, ph2

    n1, n2 = gathers(0, gn)
    e1, e2 = gathers(1, gd)

    for h in range(2):
        for hf, v in x2[h].finish():
            own[0, h, :, hf] = v.astype(F32)
    ss = jnp.zeros((tb, 1), F32)
    for h in range(2):
        v = own[0, h]
        ss = ss + jnp.sum(v * v, axis=-1, keepdims=True)
    rs = lax.rsqrt(ss / d + EPS)
    for h in range(2):
        gf = g_ref[:, pl.ds(h * dh, dh)].astype(F32)
        gn[h, c, y, x] = (own[0, h] * rs * gf).astype(BF16)
        n1[h].start()
    for h in range(2):
        v = own[0, h]
        for m in range(k):
            x_ref[m, :, pl.ds(h * dh, dh)] = v[m * tl:(m + 1) * tl].astype(BF16)

    for h in range(2):
        for hf, v in d2[h].finish():
            own[1, h, :, hf] = v
    dot = jnp.zeros((tb, 1), F32)
    for h in range(2):
        gf = g_ref[:, pl.ds(h * dh, dh)].astype(F32)
        nh = own[0, h] * rs
        dot = dot + jnp.sum(nh * (gf * own[1, h]), axis=-1, keepdims=True)
    dot = dot / d
    for h in range(2):
        gf = g_ref[:, pl.ds(h * dh, dh)].astype(F32)
        nh = own[0, h] * rs
        dxn = rs * (gf * own[1, h] - nh * dot)
        dr = jnp.concatenate([dres_ref[m, :, pl.ds(h * dh, dh)].astype(F32) for m in range(k)], axis=0)
        gd[h, c, y, x] = (dr + dxn).astype(BF16)
        e1[h].start()
    for h in range(2):
        dgp[:, pl.ds(h * dh, dh)] = jnp.sum(own[1, h] * (own[0, h] * rs), axis=0, keepdims=True)
    dgpair = remote(dgp, dgs, dg_s.at[0], dg_r.at[0], sib)

    for h in range(2):
        n1[h].mid()
    for h in range(2):
        e1[h].mid()

    def spread(buf, axis, base):
        return [remote(buf.at[coord[axis]], buf.at[coord[axis]], dg_s.at[base + i], dg_r.at[base + i],
                       peer(axis, s)) for i, s in enumerate((1, -1, 2))]

    def total(buf):
        v = buf[0]
        for i in range(1, n):
            v = v + buf[i]
        return v

    dgpair.wait_recv()
    dgx[x] = dgp[...] + dgs[...]
    sx = spread(dgx, "x", 1)
    for h in range(2):
        n1[h].finish()
        n2[h].start()
    for h in range(2):
        e1[h].finish()
        e2[h].start()
    for cp in sx:
        cp.wait_recv()
    dgy[y] = total(dgx)
    sy = spread(dgy, "y", 4)
    for h in range(2):
        n2[h].mid()
    for h in range(2):
        e2[h].mid()

    outs = []

    def put(st, g, out, cc, i):
        cp = pltpu.make_async_copy(g.at[:, cc], out.at[:, cc], osem.at[st, i])
        cp.start()
        outs.append(cp)

    def to_sib(st, g):
        return [remote(g.at[h, c], g.at[h, c], sib_s.at[st, h], sib_r.at[st, h], sib) for h in range(2)]

    for h in range(2):
        n2[h].finish()
    bn = to_sib(0, gn)
    put(0, gn, nall_ref, c, 0)
    for cp in sy:
        cp.wait_recv()
    dg_ref[...] = total(dgy)
    for h in range(2):
        e2[h].finish()
    bd = to_sib(1, gd)
    put(1, gd, dxall_ref, c, 0)
    for cp in bn:
        cp.wait_recv()
    put(0, gn, nall_ref, 1 - c, 1)
    for cp in bd:
        cp.wait_recv()
    put(1, gd, dxall_ref, 1 - c, 1)
    for cp in sends:
        cp.wait_send()
    for cp in outs:
        cp.wait()


def tail_kernel(dims, loc_ref, n_ref, dx_ref, w_ref, du_ref, u_ref, de_ref, dw_ref, oh, dup, uacc):
    k, tl, side = dims["k"], dims["tl"], dims["n"]
    tb = k * tl
    j = pl.program_id(0)
    step = min(256, oh.shape[0])

    @pl.when(j == 0)
    def _():
        @pl.loop(0, oh.shape[0] // step)
        def _(i):
            ids = lax.broadcasted_iota(jnp.int32, (step, oh.shape[1]), 0) + i * step
            oh[pl.ds(pl.multiple_of(i * step, step), step), :] = (ids == loc_ref[...]).astype(BF16)

        duf = [du_ref[m].astype(F32) for m in range(k)]
        for cc in range(2):
            for b in range(side * side):
                r = b * 2 + cc
                blk = jnp.concatenate([v[r * tl:(r + 1) * tl] for v in duf], axis=0)
                dup[pl.ds((cc * side * side + b) * tb, tb), :] = blk.astype(BF16)
        uacc[...] = jnp.zeros_like(uacc)

    nv = n_ref[0]
    de_ref[...] = jnp.dot(oh[...], dx_ref[0], preferred_element_type=F32)
    dw_ref[...] = lax.dot_general(nv, dup[...], (((0,), (0,)), ((), ())), preferred_element_type=F32)
    uacc[...] += jnp.dot(nv, w_ref[...], preferred_element_type=F32)

    @pl.when(j == pl.num_programs(0) - 1)
    def _():
        for m in range(k):
            parts = []
            for b in range(side * side):
                for cc in range(2):
                    row = (cc * side * side + b) * tb + m * tl
                    parts.append(uacc[pl.ds(row, tl), :])
            u_ref[m] = jnp.concatenate(parts, axis=0).astype(BF16)


def solution(mesh):
    groups = mesh.shape["tp"]
    side = math.isqrt(groups // 2)

    def local(ids, emb, g, w, du, dres):
        r = lax.axis_index("tp")
        k, t = ids.shape
        vl, d = emb.shape
        f = w.shape[1]
        tl = t // groups
        tb = k * tl
        n = side
        dh, dq = d // 2, d // 4
        cw = 256 if dh % 256 == 0 else 128
        nch = dh // cw
        dims = dict(k=k, tl=tl, d=d, n=n, cw=cw)
        loc = ids.reshape(k, n, n, 2, tl).transpose(3, 1, 2, 0, 4).reshape(-1) - r * vl
        hbm = pl.BlockSpec(memory_space=pl.ANY)
        vm = pl.BlockSpec(memory_space=pltpu.VMEM)
        gshape = (2, 2, n, n, tb, dh)
        xo, nall, dxall, dg = pl.pallas_call(
            functools.partial(comm_kernel, dims),
            out_shape=[
                jax.ShapeDtypeStruct((k, tl, d), BF16),
                jax.ShapeDtypeStruct(gshape, BF16),
                jax.ShapeDtypeStruct(gshape, BF16),
                jax.ShapeDtypeStruct((1, d), F32),
            ],
            in_specs=[vm, hbm, vm, vm, vm, vm],
            out_specs=[vm, hbm, hbm, vm],
            scratch_shapes=[
                VMEM((2, vl, dh), BF16), DMA((2,)),
                VMEM((k * t, f), BF16), VMEM((k * t, vl), BF16),
                VMEM((2, 2, n, n * tb, dh), BF16), VMEM((2, n, n * tb, dh), BF16),
                VMEM((2, n, n * tb, dh), F32), VMEM((2, 3, 2, n * tb, dq), F32),
                VMEM((2, n, tb, dh), F32), VMEM((2, 3, 2, tb, dq), F32),
                VMEM((2, 2, n, n * tb, dh), BF16), VMEM((2, n, n * tb, dh), BF16),
                VMEM((2, 3, 2, n * tb, dq), BF16),
                VMEM((2, n, tb, dh), BF16), VMEM((2, 3, 2, tb, dq), BF16),
                VMEM((2, 2, tb, dh), F32), VMEM(gshape, BF16), VMEM(gshape, BF16),
                VMEM((1, d), F32), VMEM((1, d), F32), VMEM((n, 1, d), F32), VMEM((n, 1, d), F32),
                DMA((2, 2)), DMA((2, 2)),
                DMA((2, 2, 2, 3, 2)), DMA((2, 2, 2, 3, 2)),
                DMA((2, 2, 2, 2, 2)), DMA((2, 2, 2, 2, 2)),
                DMA((2, 2)), DMA((2, 2)),
                DMA((7,)), DMA((7,)), DMA((2, 2)),
            ],
            compiler_params=pltpu.CompilerParams(collective_id=0, has_side_effects=True,
                                                 vmem_limit_bytes=62 * 1024 * 1024),
        )(loc[:, None], emb, g[None, :], w, du, dres)
        u, de, dw = pl.pallas_call(
            functools.partial(tail_kernel, dims),
            grid=(2 * nch,),
            out_shape=[
                jax.ShapeDtypeStruct((k, t, f), BF16),
                jax.ShapeDtypeStruct((vl, d), F32),
                jax.ShapeDtypeStruct((d, f), F32),
            ],
            in_specs=[
                pl.BlockSpec((1, k * t), lambda j: (0, 0)),
                pl.BlockSpec((1, k * t, cw), lambda j: (j // nch, 0, j % nch)),
                pl.BlockSpec((1, k * t, cw), lambda j: (j // nch, 0, j % nch)),
                pl.BlockSpec((cw, f), lambda j: (j, 0)),
                pl.BlockSpec((k, t, f), lambda j: (0, 0, 0)),
            ],
            out_specs=[
                pl.BlockSpec((k, t, f), lambda j: (0, 0, 0)),
                pl.BlockSpec((vl, cw), lambda j: (0, j)),
                pl.BlockSpec((cw, f), lambda j: (j, 0)),
            ],
            scratch_shapes=[VMEM((vl, k * t), BF16), VMEM((k * t, f), BF16), VMEM((k * t, f), F32)],
        )(loc[None, :], nall.reshape(2, k * t, dh), dxall.reshape(2, k * t, dh), w, du)
        return u, xo, de, dw, dg.reshape(d)

    return jax.shard_map(
        local,
        mesh=mesh,
        in_specs=(P("dp", None), P("tp", None), P(None), P(None, "tp"), P("dp", None, "tp"), P("dp", "tp", None)),
        out_specs=(P("dp", None, "tp"), P("dp", "tp", None), P(("dp", "tp"), None), P(None, ("dp", "tp")), P("dp")),
        check_vma=False,
    )
```

```python
import functools
import math

import jax
import jax.numpy as jnp
from jax import lax
from jax.experimental import pallas as pl
from jax.experimental.pallas import tpu as pltpu
from jax.sharding import PartitionSpec as P

EPS = 1e-6
F32 = jnp.float32
BF16 = jnp.bfloat16
VMEM = pltpu.VMEM
DMA = pltpu.SemaphoreType.DMA


def comm_kernel(dims, ids_ref, emb_ref, g_ref, w_ref, du_ref, dres_ref,
                x_ref, nall_ref, dxall_ref, dg_ref, tab_ref,
                ebuf, esem, oh, pdn, rpdn, s1, r1, t1, r2, xp, rxp, rx1, tx, rx2,
                own, gn, gd, dgp, dgs, dgx, dgy,
                pair_s, pair_r, rs_s, rs_r, ag_s, ag_r, sib_s, sib_r, dg_s, dg_r, osem):
    k, tl, d, n = dims["k"], dims["tl"], dims["d"], dims["n"]
    dh, dq, cw = d // 2, d // 4, dims["cw"]
    nch = dh // cw
    tb = k * tl
    t = du_ref.shape[1]
    vl = emb_ref.shape[0]
    me = lax.axis_index("tp")
    c = lax.rem(me, 2)
    x = lax.rem(me // 2, n)
    y = me // (2 * n)

    def dev(yy, xx, cc):
        return {"tp": (yy * n + xx) * 2 + cc}

    def add(v, s):
        return lax.rem(v + s + n, n)

    coord = {"x": x, "y": y}

    def peer(axis, s):
        return dev(y, add(x, s), c) if axis == "x" else dev(add(y, s), x, c)

    gall = g_ref[...].astype(F32).reshape(1, d)
    sib = dev(y, x, 1 - c)
    sends = []

    def remote(src, dst, ss, rs, to):
        cp = pltpu.make_async_remote_copy(src_ref=src, dst_ref=dst, send_sem=ss, recv_sem=rs,
                                          device_id=to, device_id_type=pl.DeviceIdType.MESH)
        cp.start()
        sends.append(cp)
        return cp

    barrier = pltpu.get_barrier_semaphore()
    greet = [sib] + [peer(a, s) for a in ("x", "y") for s in (1, -1, 2)]
    for to in greet:
        pl.semaphore_signal(barrier, inc=1, device_id=to, device_id_type=pl.DeviceIdType.MESH)

    eload = []
    for h in range(2):
        cp = pltpu.make_async_copy(emb_ref.at[:, pl.ds(h * dh, dh)], ebuf.at[h], esem.at[h])
        cp.start()
        eload.append(cp)

    def scatter_rows(dst, h, j, val):
        cols = pl.ds(pl.multiple_of(j * cw, cw), cw)
        for cc in range(2):
            for yy in range(n):
                for xx in range(n):
                    p, q = (xx, yy) if h == 0 else (yy, xx)
                    row = ((yy * n + xx) * 2 + cc) * tl
                    blk = jnp.concatenate([val[m * t + row:m * t + row + tl] for m in range(k)], axis=0)
                    dst[h, cc, p, pl.ds(q * tb, tb), cols] = blk.astype(BF16)

    for h in range(2):
        @pl.loop(0, nch)
        def _(j):
            wj = w_ref[pl.ds(pl.multiple_of(h * dh + j * cw, cw), cw), :]
            v = lax.dot_general(du_ref[...].reshape(k * t, -1), wj,
                                (((1,), (1,)), ((), ())), preferred_element_type=F32)
            scatter_rows(pdn, h, j, v)

    pl.semaphore_wait(barrier, len(greet))
    pair = [remote(pdn.at[h, 1 - c], rpdn.at[h], pair_s.at[0, h], pair_r.at[0, h], sib) for h in range(2)]

    loc = ids_ref[...] - me * vl
    locp = jnp.concatenate([loc, jnp.zeros((8 - k, t), jnp.int32)], axis=0) if k < 8 else loc
    loct = jnp.transpose(locp)
    step = 64
    ids = lax.broadcasted_iota(jnp.int32, (step, vl), 1)
    for m in range(k):
        for i in range(t // step):
            rows = pl.ds(m * t + i * step, step)
            oh[rows, :] = (loct[i * step:(i + 1) * step, m:m + 1] == ids).astype(BF16)

    nt = k * t
    keyc = jnp.concatenate([loct[:, m:m + 1] for m in range(k)], axis=0)
    keyr = jnp.concatenate([loc[m:m + 1] for m in range(k)], axis=1)
    posc = lax.broadcasted_iota(jnp.int32, (nt, 1), 0)
    posr = lax.broadcasted_iota(jnp.int32, (1, nt), 1)
    okr = (keyr >= 0) & (keyr < vl)
    okc = (keyc >= 0) & (keyc < vl)
    sortr = jnp.where(okr, keyr, vl) * nt + posr
    sortc = jnp.where(okc, keyc, vl) * nt + posc
    rank = jnp.sum((sortr < sortc).astype(F32), axis=1, keepdims=True)
    hit = rank == posr.astype(F32)
    tok = posc % t
    blk = tok // tl
    place = ((blk % 2) * n * n + blk // 2) * tb + (posc // t) * tl + tok % tl
    tab_ref[0:1, :] = jnp.sum(jnp.where(hit, keyc.astype(F32), 0.0), axis=0, keepdims=True).astype(jnp.int32)
    tab_ref[1:2, :] = jnp.sum(jnp.where(hit, place.astype(F32), 0.0), axis=0, keepdims=True).astype(jnp.int32)
    below = okc & (keyc < posr * dims["rt"])
    tab_ref[2:3, :] = jnp.sum(below.astype(F32), axis=0, keepdims=True).astype(jnp.int32)

    class Ring:
        def __init__(self, sem, axis, s, r):
            self.sem, self.axis, self.s, self.r = sem, axis, s, r
            self.p = coord[axis]

        def half(self, sgn):
            return pl.ds(0 if sgn > 0 else dq, dq)

        def send(self, msg, sgn, block, half):
            i = 0 if sgn > 0 else 1
            st, h, ph = self.sem
            return remote(self.s.at[block, :, half], self.r.at[msg, i],
                          rs_s.at[st, h, ph, msg, i], rs_r.at[st, h, ph, msg, i], peer(self.axis, sgn))

        def start(self):
            self.a1 = [self.send(0, sg, add(self.p, 2), self.half(sg)) for sg in (1, -1)]
            self.a2 = [self.send(1, sg, add(self.p, sg), self.half(-sg)) for sg in (1, -1)]

        def mid(self):
            self.b = []
            for i, sg in enumerate((1, -1)):
                self.a1[i].wait_recv()
                blk, hf = add(self.p, sg), self.half(sg)
                self.s[blk, :, hf] = self.s[blk, :, hf] + self.r[0, i]
                self.b.append(self.send(2, sg, blk, hf))

        def finish(self):
            for cp in self.a2 + self.b:
                cp.wait_recv()
            for i, sg in enumerate((1, -1)):
                hf = self.half(sg)
                yield hf, self.s[self.p, :, hf] + self.r[2, i] + self.r[1, 1 - i]

    axes = [("x", "y"), ("y", "x")]

    def first(st, h, s, r):
        return Ring((st, h, 0), axes[h][0], s, r.at[h])

    def second(st, h, t, r):
        return Ring((st, h, 1), axes[h][1], t.at[h], r.at[h])

    d1 = [first(0, h, s1.at[h], r1) for h in range(2)]
    d2 = [second(0, h, t1, r2) for h in range(2)]
    x1 = [first(1, h, xp.at[h, c], rx1) for h in range(2)]
    x2 = [second(1, h, tx, rx2) for h in range(2)]

    def finish1(ring, t, h):
        for hf, v in ring.finish():
            t[h, :, :, hf] = v.reshape(n, tb, dq)

    def emm(h, lo, hi):
        @pl.loop(lo, hi)
        def _(j):
            ej = ebuf[h, :, pl.ds(pl.multiple_of(j * cw, cw), cw)]
            v = jnp.dot(oh[...], ej, preferred_element_type=F32)
            scatter_rows(xp, h, j, v)

    def start_d1(h):
        pair[h].wait_recv()
        for p in range(n):
            s1[h, p] = pdn[h, c, p].astype(F32) + rpdn[h, p].astype(F32)
        d1[h].start()

    def send_x(h):
        return remote(xp.at[h, 1 - c], rxp.at[h], pair_s.at[1, h], pair_r.at[1, h], sib)

    def start_x1(h):
        xpair[h].wait_recv()
        for p in range(n):
            xp[h, c, p] = xp[h, c, p] + rxp[h, p]
        x1[h].start()

    cuts = [nch // 7, 2 * nch // 7, 3 * nch // 7]
    eload[0].wait()
    emm(0, 0, cuts[0])
    start_d1(0)
    emm(0, cuts[0], cuts[1])
    start_d1(1)
    emm(0, cuts[1], nch)
    xpair = [send_x(0)]
    eload[1].wait()
    emm(1, 0, cuts[2])
    start_x1(0)
    emm(1, cuts[2], nch)
    xpair.append(send_x(1))
    for h in range(2):
        d1[h].mid()
    start_x1(1)
    for h in range(2):
        x1[h].mid()
    finish1(x1[0], tx, 0)
    x2[0].start()
    finish1(d1[0], t1, 0)
    d2[0].start()
    finish1(x1[1], tx, 1)
    x2[1].start()
    finish1(d1[1], t1, 1)
    d2[1].start()
    for h in range(2):
        x2[h].mid()
    for h in range(2):
        d2[h].mid()

    outs = []

    class Gather:
        def __init__(self, sem, axis, get, put=None):
            self.sem, self.axis, self.get, self.put = sem, axis, get, put
            self.p = coord[axis]
            self.sibs = []

        def send(self, msg, sgn, block, half):
            i = 0 if sgn > 0 else 1
            st, h, ph = self.sem
            ref = self.get(c, block, half)
            return remote(ref, ref, ag_s.at[st, h, ph, msg, i], ag_r.at[st, h, ph, msg, i],
                          peer(self.axis, sgn))

        def have(self, s):
            if self.put is None:
                return
            st, h, _ = self.sem
            i = s % n
            ref = self.get(c, add(self.p, s), pl.ds(0, dh))
            self.sibs.append((s, remote(ref, ref, sib_s.at[st, h, i], sib_r.at[st, h, i], sib)))
            self.out(c, s, 0)

        def out(self, cc, s, side):
            st, h, _ = self.sem
            block = add(self.p, s)
            cp = pltpu.make_async_copy(self.get(cc, block, pl.ds(0, dh)), self.put(cc, block),
                                       osem.at[st, h, side, s % n])
            cp.start()
            outs.append(cp)

        def start(self):
            self.a = [self.send(0, sg, self.p, pl.ds(0, dh)) for sg in (1, -1)]
            self.have(0)

        def mid(self):
            self.b = []
            for i, sg in enumerate((1, -1)):
                self.a[i].wait_recv()
                self.b.append(self.send(1, sg, add(self.p, -sg), pl.ds(0 if sg > 0 else dq, dq)))
                self.have(-sg)

        def finish(self):
            for cp in self.b:
                cp.wait_recv()
            self.have(2)

        def drain(self, count):
            for s, cp in self.sibs[:count]:
                cp.wait_recv()
                self.out(1 - c, s, 1)
            self.sibs = self.sibs[count:]

    def gathers(st, g, out):
        ph1, ph2 = [], []
        c0, c1 = pl.ds(0, dh), pl.ds(dh, dh)
        ph1.append(Gather((st, 0, 0), "x", lambda cc, i, hf: g.at[0, cc, y, i, :, hf]))
        ph2.append(Gather((st, 0, 1), "y", lambda cc, i, hf: g.at[0, cc, i, :, :, hf],
                          lambda cc, i: out.at[cc, i, :, :, c0]))
        ph1.append(Gather((st, 1, 0), "y", lambda cc, i, hf: g.at[1, cc, i, x, :, hf]))
        ph2.append(Gather((st, 1, 1), "x", lambda cc, i, hf: g.at[1, cc, :, i, :, hf],
                          lambda cc, i: out.at[cc, :, i, :, c1]))
        return ph1, ph2

    n1, n2 = gathers(0, gn, nall_ref)
    e1, e2 = gathers(1, gd, dxall_ref)

    for h in range(2):
        for hf, v in x2[h].finish():
            own[0, h, :, hf] = v.astype(F32)
    ss = jnp.zeros((tb, 1), F32)
    for h in range(2):
        v = own[0, h]
        ss = ss + jnp.sum(v * v, axis=-1, keepdims=True)
    rs = lax.rsqrt(ss / d + EPS)
    for h in range(2):
        gf = gall[:, h * dh:(h + 1) * dh]
        gn[h, c, y, x] = (own[0, h] * rs * gf).astype(BF16)
        n1[h].start()
    for h in range(2):
        v = own[0, h]
        for m in range(k):
            x_ref[m, :, pl.ds(h * dh, dh)] = v[m * tl:(m + 1) * tl].astype(BF16)

    for h in range(2):
        for hf, v in d2[h].finish():
            own[1, h, :, hf] = v
    dot = jnp.zeros((tb, 1), F32)
    for h in range(2):
        gf = gall[:, h * dh:(h + 1) * dh]
        nh = own[0, h] * rs
        dot = dot + jnp.sum(nh * (gf * own[1, h]), axis=-1, keepdims=True)
    dot = dot / d
    for h in range(2):
        gf = gall[:, h * dh:(h + 1) * dh]
        nh = own[0, h] * rs
        dxn = rs * (gf * own[1, h] - nh * dot)
        dr = jnp.concatenate([dres_ref[m, :, pl.ds(h * dh, dh)].astype(F32) for m in range(k)], axis=0)
        gd[h, c, y, x] = (dr + dxn).astype(BF16)
        e1[h].start()
    for h in range(2):
        dgp[:, pl.ds(h * dh, dh)] = jnp.sum(own[1, h] * (own[0, h] * rs), axis=0, keepdims=True)
    dgpair = remote(dgp, dgs, dg_s.at[0], dg_r.at[0], sib)

    for h in range(2):
        n1[h].mid()
    for h in range(2):
        e1[h].mid()

    def spread(buf, axis, base):
        return [remote(buf.at[coord[axis]], buf.at[coord[axis]], dg_s.at[base + i], dg_r.at[base + i],
                       peer(axis, s)) for i, s in enumerate((1, -1, 2))]

    def total(buf):
        v = buf[0]
        for i in range(1, n):
            v = v + buf[i]
        return v

    dgpair.wait_recv()
    dgx[x] = dgp[...] + dgs[...]
    sx = spread(dgx, "x", 1)
    for h in range(2):
        n1[h].finish()
        n2[h].start()
    for h in range(2):
        e1[h].finish()
        e2[h].start()
    for cp in sx:
        cp.wait_recv()
    dgy[y] = total(dgx)
    sy = spread(dgy, "y", 4)
    for h in range(2):
        n2[h].mid()
    for h in range(2):
        e2[h].mid()

    for h in range(2):
        n2[h].finish()
    for cp in sy:
        cp.wait_recv()
    dg_ref[...] = total(dgy).reshape(d)
    for h in range(2):
        n2[h].drain(4)
    for h in range(2):
        e2[h].drain(1)
    for h in range(2):
        e2[h].finish()
    for i in (2, 1):
        for h in range(2):
            e2[h].drain(i)
    for cp in sends:
        cp.wait_send()
    for cp in outs:
        cp.wait()


def tail_kernel(dims, tab_ref, n_ref, dx_ref, w_ref, du_ref, x_ref, dg_ref,
                u_ref, de_ref, dw_ref, xo_ref, dgo_ref, dxf, dup, uacc):
    k, tl, side = dims["k"], dims["tl"], dims["n"]
    tb = k * tl
    rt = dims["rt"]
    j = pl.program_id(0)

    @pl.when(j == 0)
    def _():
        dxf[...] = dx_ref[...].astype(F32)

    de_ref[...] = jnp.zeros_like(de_ref)

    @pl.loop(tab_ref[2, j], tab_ref[2, j + 1])
    def _(i):
        row = pl.ds(tab_ref[0, i] - j * rt, 1)
        de_ref[row, :] = de_ref[row, :] + dxf[pl.ds(tab_ref[1, i], 1), :]

    @pl.when(j == 0)
    def _():
        duf = [du_ref[m].astype(F32) for m in range(k)]
        for cc in range(2):
            for b in range(side * side):
                r = b * 2 + cc
                blk = jnp.concatenate([v[r * tl:(r + 1) * tl] for v in duf], axis=0)
                dup[pl.ds((cc * side * side + b) * tb, tb), :] = blk.astype(BF16)
        uacc[...] = jnp.zeros_like(uacc)
        xo_ref[...] = x_ref[...]
        dgo_ref[...] = dg_ref[...]

    @pl.when((j > 0) & (j <= dims["nw"]))
    def _():
        nv = n_ref[...]
        dw_ref[...] = lax.dot_general(nv, dup[...], (((0,), (0,)), ((), ())), preferred_element_type=F32)
        uacc[...] += jnp.dot(nv, w_ref[...], preferred_element_type=F32)

    @pl.when(j == pl.num_programs(0) - 1)
    def _():
        for m in range(k):
            parts = []
            for b in range(side * side):
                for cc in range(2):
                    row = (cc * side * side + b) * tb + m * tl
                    parts.append(uacc[pl.ds(row, tl), :])
            u_ref[m] = jnp.concatenate(parts, axis=0).astype(BF16)


def solution(mesh):
    groups = mesh.shape["tp"]
    side = math.isqrt(groups // 2)

    def local(ids, emb, g, w, du, dres):
        k, t = ids.shape
        vl, d = emb.shape
        f = w.shape[1]
        tl = t // groups
        tb = k * tl
        n = side
        dh, dq = d // 2, d // 4
        cw = 256 if dh % 256 == 0 else 128
        rt = vl // 8
        wc = d // 7 if d % 896 == 0 else d // 4
        nw = d // wc
        dims = dict(k=k, tl=tl, d=d, n=n, cw=cw, rt=rt, nw=nw)
        hbm = pl.BlockSpec(memory_space=pl.ANY)
        vm = pl.BlockSpec(memory_space=pltpu.VMEM)
        gshape = (2, 2, n, n, tb, dh)
        oshape = (2, n, n, tb, d)
        xo, nall, dxall, dg, tab = pl.pallas_call(
            functools.partial(comm_kernel, dims),
            out_shape=[
                jax.ShapeDtypeStruct((k, tl, d), BF16),
                jax.ShapeDtypeStruct(oshape, BF16),
                jax.ShapeDtypeStruct(oshape, BF16),
                jax.ShapeDtypeStruct((d,), F32),
                jax.ShapeDtypeStruct((8, k * t), jnp.int32),
            ],
            in_specs=[vm, hbm, vm, vm, vm, vm],
            out_specs=[vm, hbm, hbm, vm, vm],
            scratch_shapes=[
                VMEM((2, vl, dh), BF16), DMA((2,)),
                VMEM((k * t, vl), BF16),
                VMEM((2, 2, n, n * tb, dh), BF16), VMEM((2, n, n * tb, dh), BF16),
                VMEM((2, n, n * tb, dh), F32), VMEM((2, 3, 2, n * tb, dq), F32),
                VMEM((2, n, tb, dh), F32), VMEM((2, 3, 2, tb, dq), F32),
                VMEM((2, 2, n, n * tb, dh), BF16), VMEM((2, n, n * tb, dh), BF16),
                VMEM((2, 3, 2, n * tb, dq), BF16),
                VMEM((2, n, tb, dh), BF16), VMEM((2, 3, 2, tb, dq), BF16),
                VMEM((2, 2, tb, dh), F32), VMEM(gshape, BF16), VMEM(gshape, BF16),
                VMEM((1, d), F32), VMEM((1, d), F32), VMEM((n, 1, d), F32), VMEM((n, 1, d), F32),
                DMA((2, 2)), DMA((2, 2)),
                DMA((2, 2, 2, 3, 2)), DMA((2, 2, 2, 3, 2)),
                DMA((2, 2, 2, 2, 2)), DMA((2, 2, 2, 2, 2)),
                DMA((2, 2, n)), DMA((2, 2, n)),
                DMA((7,)), DMA((7,)), DMA((2, 2, 2, n)),
            ],
            compiler_params=pltpu.CompilerParams(collective_id=0, has_side_effects=True,
                                                 vmem_limit_bytes=62 * 1024 * 1024),
        )(ids, emb, g, w, du, dres)
        u, de, dw, xo, dg = pl.pallas_call(
            functools.partial(tail_kernel, dims),
            grid=(vl // rt,),
            out_shape=[
                jax.ShapeDtypeStruct((k, t, f), BF16),
                jax.ShapeDtypeStruct((vl, d), F32),
                jax.ShapeDtypeStruct((d, f), F32),
                jax.ShapeDtypeStruct((k, tl, d), BF16),
                jax.ShapeDtypeStruct((d,), F32),
            ],
            in_specs=[
                pl.BlockSpec(memory_space=pltpu.SMEM),
                pl.BlockSpec((k * t, wc), lambda j: (0, jnp.clip(j - 1, 0, nw - 1))),
                pl.BlockSpec((k * t, d), lambda j: (0, 0), pipeline_mode=pl.Buffered(1)),
                pl.BlockSpec((wc, f), lambda j: (jnp.clip(j - 1, 0, nw - 1), 0)),
                pl.BlockSpec((k, t, f), lambda j: (0, 0, 0)),
                pl.BlockSpec((k, tl, d), lambda j: (0, 0, 0)),
                pl.BlockSpec((d,), lambda j: (0,)),
            ],
            out_specs=[
                pl.BlockSpec((k, t, f), lambda j: (0, 0, 0)),
                pl.BlockSpec((rt, d), lambda j: (j, 0)),
                pl.BlockSpec((wc, f), lambda j: (jnp.clip(j - 1, 0, nw - 1), 0)),
                pl.BlockSpec((k, tl, d), lambda j: (0, 0, 0)),
                pl.BlockSpec((d,), lambda j: (0,)),
            ],
            scratch_shapes=[VMEM((k * t, d), F32), VMEM((k * t, f), BF16), VMEM((k * t, f), F32)],
            compiler_params=pltpu.CompilerParams(vmem_limit_bytes=62 * 1024 * 1024),
        )(tab, nall.reshape(k * t, d), dxall.reshape(k * t, d), w, du, xo, dg)
        return u, xo, de, dw, dg

    return jax.shard_map(
        local,
        mesh=mesh,
        in_specs=(P("dp", None), P("tp", None), P(None), P(None, "tp"), P("dp", None, "tp"), P("dp", "tp", None)),
        out_specs=(P("dp", None, "tp"), P("dp", "tp", None), P(("dp", "tp"), None), P(None, ("dp", "tp")), P("dp")),
        check_vma=False,
    )
```

```python
import functools
import math

import jax
import jax.numpy as jnp
from jax import lax
from jax.experimental import pallas as pl
from jax.experimental.pallas import tpu as pltpu
from jax.sharding import PartitionSpec as P

EPS = 1e-6
F32 = jnp.float32
BF16 = jnp.bfloat16
VMEM = pltpu.VMEM
DMA = pltpu.SemaphoreType.DMA
BOTH = range(2)
WAYS = (1, -1)
SHIFTS = (2, 1, -1)
RING = {(0, 0): 0, (0, 1): 5, (1, 1): 8}


def comm_kernel(dims, ids_ref, emb_ref, g_ref, w_ref, du_ref, dres_ref,
                xout_ref, nall_ref, dxall_ref, dgout_ref, tabout_ref,
                ebuf, esem, oh, pdn, rpdn, s1, r1, t1, r2, xp, rxp, rx1, tx, rx2,
                own, gn, gd, dgp, dgs, dgx, dgy,
                pair_s, pair_r, rs_s, rs_r, ag_s, ag_r, sib_s, sib_r, dg_s, dg_r, osem,
                xc, rxc, rq, cc_e, fx, hop_s, hop_r, x_ref, dg_ref, tab_ref, small_sem):
    k, tl, d, n, fast = dims["k"], dims["tl"], dims["d"], dims["n"], dims["fast"]
    dh, dq, cw = d // 2, d // 4, dims["cw"]
    nch = dh // cw
    cb = dims["cb"]
    tb = k * tl
    t = du_ref.shape[1]
    vl = emb_ref.shape[0]
    me = lax.axis_index("tp")
    c = lax.rem(me, 2)
    x = lax.rem(me // 2, n)
    y = me // (2 * n)

    def dev(yy, xx, cc):
        return {"tp": (yy * n + xx) * 2 + cc}

    def add(v, s):
        return lax.rem(v + s + n, n)

    coord = {"x": x, "y": y}

    def peer(axis, s):
        return dev(y, add(x, s), c) if axis == "x" else dev(add(y, s), x, c)

    gall = g_ref[...].astype(F32).reshape(1, d)
    sib = dev(y, x, 1 - c)
    sends, outs = [], []

    def emit(i, src, dst):
        cp = pltpu.make_async_copy(src, dst, small_sem.at[i])
        cp.start()
        outs.append(cp)

    def remote(src, dst, ss, rs, to):
        cp = pltpu.make_async_remote_copy(src_ref=src, dst_ref=dst, send_sem=ss, recv_sem=rs,
                                          device_id=to, device_id_type=pl.DeviceIdType.MESH)
        cp.start()
        sends.append(cp)
        return cp

    barrier = pltpu.get_barrier_semaphore()
    greet = [sib] + [peer(a, s) for a in ("x", "y") for s in (1, -1, 2)]
    for to in greet:
        pl.semaphore_signal(barrier, inc=1, device_id=to, device_id_type=pl.DeviceIdType.MESH)

    eload = []
    for h in BOTH:
        cp = pltpu.make_async_copy(emb_ref.at[:, pl.ds(h * dh, dh)], ebuf.at[h], esem.at[h])
        cp.start()
        eload.append(cp)

    def scatter_rows(dst, h, j, val, cw):
        cols = pl.ds(pl.multiple_of(j * cw, cw), cw)
        for cc in BOTH:
            for yy in range(n):
                for xx in range(n):
                    p, q = (xx, yy) if h == 0 else (yy, xx)
                    row = ((yy * n + xx) * 2 + cc) * tl
                    blk = jnp.concatenate([val[m * t + row:m * t + row + tl] for m in range(k)], axis=0)
                    dst[h, cc, p, pl.ds(q * tb, tb), cols] = blk.astype(BF16)

    for h in BOTH:
        @pl.loop(0, dh // cb)
        def _(j):
            wj = w_ref[pl.ds(pl.multiple_of(h * dh + j * cb, cb), cb), :]
            v = lax.dot_general(du_ref[...].reshape(k * t, -1), wj,
                                (((1,), (1,)), ((), ())), preferred_element_type=F32)
            scatter_rows(pdn, h, j, v, cb)

    pl.semaphore_wait(barrier, len(greet))
    pair = [remote(pdn.at[h, 1 - c], rpdn.at[h], pair_s.at[0, h], pair_r.at[0, h], sib) for h in BOTH]

    loc = ids_ref[...] - me * vl
    locp = jnp.concatenate([loc, jnp.zeros((8 - k, t), jnp.int32)], axis=0) if k < 8 else loc
    loct = jnp.transpose(locp)
    if not fast:
        step = 64
        ids = lax.broadcasted_iota(jnp.int32, (step, vl), 1)
        for m in range(k):
            for i in range(t // step):
                rows = pl.ds(m * t + i * step, step)
                oh[rows, :] = (loct[i * step:(i + 1) * step, m:m + 1] == ids).astype(BF16)

    nt = k * t
    keyc = jnp.concatenate([loct[:, m:m + 1] for m in range(k)], axis=0)
    keyr = jnp.concatenate([loc[m:m + 1] for m in range(k)], axis=1)
    posc = lax.broadcasted_iota(jnp.int32, (nt, 1), 0)
    posr = lax.broadcasted_iota(jnp.int32, (1, nt), 1)

    class Facts:
        def __init__(self, key, pos):
            self.loc, self.pos = key, pos
            self.tok = pos % t
            blk = self.tok // tl
            self.c, self.at = blk % 2, {"x": (blk // 2) % n, "y": blk // (2 * n)}
            self.here = (key >= 0) & (key < vl)
            self.chip = (key + me * vl) // (2 * vl)
            self.owner = {"x": self.chip % n, "y": self.chip // n}

        def group(self, axis):
            return (self.at[axis] * 2 + self.c) * (n * n) + self.chip

    fr, fc = Facts(keyr, posr), Facts(keyc, posc)

    def rank_row(axis):
        m = (fc.group(axis) == fr.group(axis)) & (posc < posr)
        return jnp.sum(m.astype(F32), axis=0, keepdims=True).astype(jnp.int32)

    def rank_col(axis):
        m = (fc.group(axis) == fr.group(axis)) & (posr < posc)
        return jnp.sum(m.astype(F32), axis=1, keepdims=True).astype(jnp.int32)

    def pick(want, value):
        m = jnp.where(want, (value + 1).astype(F32), 0.0)
        return jnp.sum(m, axis=1, keepdims=True).astype(jnp.int32) - 1

    def table():
        sortr = jnp.where(fr.here, keyr, vl) * nt + posr
        sortc = jnp.where(fc.here, keyc, vl) * nt + posc
        rank = jnp.sum((sortr < sortc).astype(F32), axis=1, keepdims=True)
        hit = rank == posr.astype(F32)
        if fast:
            places = [(fc.c * n + fc.at["y"]) * tb + rank_col("y"), (fc.c * n + fc.at["x"]) * tb + rank_col("x")]
        else:
            place = ((fc.c * n + fc.at["y"]) * n + fc.at["x"]) * tb + (posc // t) * tl + fc.tok % tl
            places = [place]
        vals = [jnp.sum(jnp.where(hit, v.astype(F32), 0.0), axis=0, keepdims=True).astype(jnp.int32)
                for v in [keyc] + places]
        tab_ref[0:1, :] = vals[0]
        tab_ref[1:2, :] = vals[1]
        tab_ref[2:3, :] = vals[-1]
        below = fc.here & (keyc < posr * dims["rt"])
        tab_ref[3:4, :] = jnp.sum(below.astype(F32), axis=0, keepdims=True).astype(jnp.int32)
        tab_ref[4:, :] = jnp.full((4, nt), not fast, jnp.int32)
        emit(0, tab_ref, tabout_ref)

    if not fast:
        table()

    class Ring:
        def __init__(self, sem, axis, s, r, parts=1):
            self.sem, self.axis, self.s, self.r, self.parts = sem, axis, s, r, parts
            self.p = coord[axis]
            self.pr = s.shape[1] // parts
            self.b = []
            self.far_in = False

        def half(self, sgn):
            return pl.ds(0 if sgn > 0 else dq, dq)

        def rows(self, part):
            return pl.ds(part * self.pr, self.pr)

        def send(self, msg, sgn, block, half, part=None):
            i = 0 if sgn > 0 else 1
            st, h, ph = self.sem
            rows = slice(None) if part is None else self.rows(part)
            sem = (h, RING[st, ph] + msg + (part or 0) * 2, i) if fast else (st, h, ph, msg, i)
            return remote(self.s.at[block, rows, half], self.r.at[msg, i, rows],
                          rs_s.at[sem], rs_r.at[sem], peer(self.axis, sgn))

        def start(self):
            self.far()
            self.near(0)

        def far(self):
            self.a1 = [self.send(0, sg, add(self.p, 2), self.half(sg)) for sg in WAYS]

        def near(self, part):
            self.b += [self.send(1, sg, add(self.p, sg), self.half(-sg), part) for sg in WAYS]

        def mid(self, part=0):
            for i, sg in enumerate(WAYS):
                if not self.far_in:
                    self.a1[i].wait_recv()
                blk, rows, hf = add(self.p, sg), self.rows(part), self.half(sg)
                self.s[blk, rows, hf] = self.s[blk, rows, hf] + self.r[0, i, rows]
                self.b.append(self.send(2, sg, blk, hf, part))
            self.far_in = True

        def finish(self):
            for cp in self.b:
                cp.wait_recv()
            for i, sg in enumerate(WAYS):
                hf = self.half(sg)
                yield hf, self.s[self.p, :, hf] + self.r[2, i] + self.r[1, 1 - i]

    axes = [("x", "y"), ("y", "x")]

    def first(st, h, s, r):
        return Ring((st, h, 0), axes[h][0], s, r.at[h], 2 if fast and st == 0 else 1)

    def second(st, h, t, r):
        return Ring((st, h, 1), axes[h][1], t.at[h], r.at[h])

    d1 = [first(0, h, s1.at[h], r1) for h in BOTH]
    d2 = [second(0, h, t1, r2) for h in BOTH]
    x1 = [first(1, h, xp.at[h, c], rx1) for h in BOTH]
    x2 = [second(1, h, tx, rx2) for h in BOTH]

    def finish1(ring, t, h):
        for hf, v in ring.finish():
            t[h, :, :, hf] = v.reshape(n, tb, dq)

    def emm(h):
        @pl.loop(0, nch)
        def _(j):
            ej = ebuf[h, :, pl.ds(pl.multiple_of(j * cw, cw), cw)]
            v = jnp.dot(oh[...], ej, preferred_element_type=F32)
            scatter_rows(xp, h, j, v, cw)

    def start_d1(h):
        pair[h].wait_recv()
        for p in range(n):
            s1[h, p] = pdn[h, c, p].astype(F32) + rpdn[h, p].astype(F32)
        d1[h].far()
        if not fast:
            d1[h].near(0)

    def send_x(h):
        src, dst = (xc.at[h, 1 - c], rxc.at[h]) if fast else (xp.at[h, 1 - c], rxp.at[h])
        return remote(src, dst, pair_s.at[1, h], pair_r.at[1, h], sib)

    def start_x1(h):
        xpair[h].wait_recv()
        for p in range(n):
            xp[h, c, p] = xp[h, c, p] + rxp[h, p]
        x1[h].start()

    class Hop:
        def __init__(self, sem, axis, src, dst):
            self.sem, self.axis, self.src, self.dst = sem, axis, src, dst
            self.p = coord[axis]

        def start(self):
            self.a = []
            for i, sh in enumerate(SHIFTS):
                sem = (*self.sem, i)
                self.a.append(remote(self.src.at[add(self.p, sh)], self.dst.at[self.p],
                                     hop_s.at[sem], hop_r.at[sem], peer(self.axis, sh)))
            self.dst[self.p] = self.src[self.p]

        def finish(self):
            for cp in self.a:
                cp.wait_recv()

    if fast:
        rank = {a: rank_row(a) for a in ("x", "y")}
        slots = 2 * n * tb
        slotc = lax.broadcasted_iota(jnp.int32, (slots, 1), 0)
        lane = lax.broadcasted_iota(jnp.int32, (slots, vl), 1)
        for h in BOTH:
            a = axes[h][0]
            slot = (fr.c * n + fr.at[a]) * tb + rank[a]
            row = pick((slot == slotc) & fr.here & (rank[a] < tb), keyr)
            oh[pl.ds(h * slots, slots), :] = (row == lane).astype(BF16)

        def pack(h):
            eload[h].wait()

            @pl.loop(0, dh // cb)
            def _(j):
                cols = pl.ds(pl.multiple_of(j * cb, cb), cb)
                v = jnp.dot(oh[pl.ds(h * slots, slots), :], ebuf[h, :, cols], preferred_element_type=F32)
                xc[h, :, :, :, cols] = v.reshape(2, n, tb, cb).astype(BF16)

        def chosen(h, fixed, mine, slot_axis, rank_axis):
            other = "y" if slot_axis == "x" else "x"
            i = lax.broadcasted_iota(jnp.int32, (n * tb, 1), 0)
            q = i // tb
            yy, xx = (mine, q) if fixed == "y" else (q, mine)
            pos = ((i % tb) // tl) * t + ((yy * n + xx) * 2 + c) * tl + i % tl
            slot = fr.owner[slot_axis] * tb + rank[rank_axis]
            val = pick((posr == pos) & (fr.owner[other] == coord[other]) & (rank[rank_axis] < tb), slot)
            return (val == lax.broadcasted_iota(jnp.int32, (n * tb, n * tb), 1)).astype(BF16)

        hx = [Hop((0, h), axes[h][0], xc.at[h, c], rq.at[h]) for h in BOTH]
        he = [Hop((1, h), axes[h][1], cc_e.at[h], fx.at[h, c]) for h in BOTH]
        pack(0)
        xpair = [send_x(0)]
        start_d1(0)
        start_d1(1)
        pack(1)
        xpair.append(send_x(1))
        for h in BOTH:
            xpair[h].wait_recv()
            xc[h, c] = xc[h, c] + rxc[h]
            hx[h].start()
        for h in BOTH:
            d1[h].near(0)
        table()
        unpack = [chosen(h, axes[h][0], coord[axes[h][0]], axes[h][0], axes[h][0]) for h in BOTH]
        repack = [chosen(h, axes[h][1], coord[axes[h][1]], axes[h][1], axes[h][1]) for h in BOTH]
        for h in BOTH:
            d1[h].mid(0)
        for h in BOTH:
            hx[h].finish()
            for q in range(0, dh, dq):
                v = jnp.dot(unpack[h], rq[h, :, :, pl.ds(q, dq)].reshape(n * tb, dq), preferred_element_type=F32)
                tx[h, :, :, pl.ds(q, dq)] = v.reshape(n, tb, dq).astype(BF16)
            x2[h].start()
        for h in BOTH:
            d1[h].mid(1)
            d1[h].near(1)
        for h in BOTH:
            x2[h].mid()
    else:
        start_d1(0)
        start_d1(1)
        xpair = []
        for h in BOTH:
            eload[h].wait()
            emm(h)
            xpair.append(send_x(h))
        start_x1(0)
        for h in BOTH:
            d1[h].mid()
        start_x1(1)
        for h in BOTH:
            x1[h].mid()
        finish1(x1[0], tx, 0)
        x2[0].start()
        finish1(d1[0], t1, 0)
        d2[0].start()
        finish1(x1[1], tx, 1)
        x2[1].start()
        finish1(d1[1], t1, 1)
        d2[1].start()
        for h in BOTH:
            x2[h].mid()
        for h in BOTH:
            d2[h].mid()

    class Gather:
        def __init__(self, sem, axis, get, put=None):
            self.sem, self.axis, self.get, self.put = sem, axis, get, put
            self.p = coord[axis]
            self.sibs, self.a = [], []

        def send(self, msg, sgn, block, half):
            i = 0 if sgn > 0 else 1
            st, h, ph = self.sem
            ref = self.get(c, block, half)
            sem = (st * 2 + ph, h, msg, i)
            return remote(ref, ref, ag_s.at[sem], ag_r.at[sem], peer(self.axis, sgn))

        def have(self, s):
            if self.put is None:
                return
            st, h, _ = self.sem
            i = s % n
            ref = self.get(c, add(self.p, s), pl.ds(0, dh))
            self.sibs.append((s, remote(ref, ref, sib_s.at[st, h, i], sib_r.at[st, h, i], sib)))
            if st or not fast:
                self.out(c, s, 0)

        def out(self, cc, s, side):
            st, h, _ = self.sem
            block = add(self.p, s)
            cp = pltpu.make_async_copy(self.get(cc, block, pl.ds(0, dh)), self.put(cc, block),
                                       osem.at[st, h, side, s % n])
            cp.start()
            outs.append(cp)

        def open(self, part):
            self.a += [self.send(part * 2, sg, self.p, pl.ds(part * dq, dq)) for sg in WAYS]

        def start(self):
            self.open(0)
            self.open(1)
            self.have(0)

        def mid(self):
            self.b = []
            for cp in self.a:
                cp.wait_recv()
            for sg in WAYS:
                self.b.append(self.send(1, sg, add(self.p, -sg), pl.ds(0 if sg > 0 else dq, dq)))
            for sg in WAYS:
                self.have(-sg)

        def finish(self):
            for cp in self.b:
                cp.wait_recv()
            self.have(2)

        def drain(self, count):
            for s, cp in self.sibs[:count]:
                cp.wait_recv()
                if not fast:
                    self.out(1 - c, s, 1)
            self.sibs = self.sibs[count:]

    def gathers(st, g, out):
        ph1, ph2 = [], []
        c0, c1 = pl.ds(0, dh), pl.ds(dh, dh)
        ph1.append(Gather((st, 0, 0), "x", lambda cc, i, hf: g.at[0, cc, y, i, :, hf]))
        ph2.append(Gather((st, 0, 1), "y", lambda cc, i, hf: g.at[0, cc, i, :, :, hf],
                          lambda cc, i: out.at[cc, i, :, :, c0]))
        ph1.append(Gather((st, 1, 0), "y", lambda cc, i, hf: g.at[1, cc, i, x, :, hf]))
        ph2.append(Gather((st, 1, 1), "x", lambda cc, i, hf: g.at[1, cc, :, i, :, hf],
                          lambda cc, i: out.at[cc, :, i, :, c1]))
        return ph1, ph2

    n1, n2 = gathers(0, gn, nall_ref)
    e1, e2 = gathers(1, gd, dxall_ref)

    for h in BOTH:
        for hf, v in x2[h].finish():
            own[0, h, :, hf] = v.astype(F32)
    ss = jnp.zeros((tb, 1), F32)
    for h in BOTH:
        v = own[0, h]
        ss = ss + jnp.sum(v * v, axis=-1, keepdims=True)
    rs = lax.rsqrt(ss / d + EPS)
    for h in BOTH:
        gf = gall[:, h * dh:(h + 1) * dh]
        gn[h, c, y, x] = (own[0, h] * rs * gf).astype(BF16)
        n1[h].start()
    for h in BOTH:
        v = own[0, h]
        for m in range(k):
            x_ref[m, :, pl.ds(h * dh, dh)] = v[m * tl:(m + 1) * tl].astype(BF16)
    emit(1, x_ref, xout_ref)

    if fast:
        for h in BOTH:
            finish1(d1[h], t1, h)
            d2[h].start()
        for h in BOTH:
            n1[h].mid()
        for h in BOTH:
            d2[h].mid()
        for h in BOTH:
            n1[h].finish()
            n2[h].open(0)

    for h in BOTH:
        for hf, v in d2[h].finish():
            own[1, h, :, hf] = v
    dot = jnp.zeros((tb, 1), F32)
    for h in BOTH:
        gf = gall[:, h * dh:(h + 1) * dh]
        nh = own[0, h] * rs
        dot = dot + jnp.sum(nh * (gf * own[1, h]), axis=-1, keepdims=True)
    dot = dot / d
    for h in BOTH:
        gf = gall[:, h * dh:(h + 1) * dh]
        nh = own[0, h] * rs
        dxn = rs * (gf * own[1, h] - nh * dot)
        dr = jnp.concatenate([dres_ref[m, :, pl.ds(h * dh, dh)].astype(F32) for m in range(k)], axis=0)
        gd[h, c, y, x] = (dr + dxn).astype(BF16)
        e1[h].start()
    for h in BOTH:
        dgp[:, pl.ds(h * dh, dh)] = jnp.sum(own[1, h] * (own[0, h] * rs), axis=0, keepdims=True)
    if fast:
        for h in BOTH:
            n2[h].open(1)
            n2[h].have(0)
    dgpair = remote(dgp, dgs, dg_s.at[0], dg_r.at[0], sib)

    if not fast:
        for h in BOTH:
            n1[h].mid()
    for h in BOTH:
        e1[h].mid()

    def spread(buf, axis, base):
        return [remote(buf.at[coord[axis]], buf.at[coord[axis]], dg_s.at[base + i], dg_r.at[base + i],
                       peer(axis, s)) for i, s in enumerate((1, -1, 2))]

    def total(buf):
        v = buf[0]
        for i in range(1, n):
            v = v + buf[i]
        return v

    if fast:
        for h in BOTH:
            n2[h].mid()
    dgpair.wait_recv()
    dgx[x] = dgp[...] + dgs[...]
    sx = spread(dgx, "x", 1)
    if not fast:
        for h in BOTH:
            n1[h].finish()
            n2[h].start()
    for h in BOTH:
        e1[h].finish()
        if not fast:
            e2[h].start()
            continue
        for q in range(0, dh, dq):
            cols = pl.ds(q, dq)
            blk = gd[0, c, y, :, :, cols] if h == 0 else gd[1, c, :, x, :, cols]
            v = lax.dot_general(repack[h], blk.reshape(n * tb, dq), (((0,), (0,)), ((), ())),
                                preferred_element_type=F32)
            cc_e[h, :, :, cols] = v.reshape(n, tb, dq).astype(BF16)
        he[h].start()
    for cp in sx:
        cp.wait_recv()
    dgy[y] = total(dgx)
    sy = spread(dgy, "y", 4)
    if not fast:
        for h in BOTH:
            n2[h].mid()
    if not fast:
        for h in BOTH:
            e2[h].mid()

    def finish_n():
        for h in BOTH:
            n2[h].finish()
        for cp in sy:
            cp.wait_recv()
        dg_ref[...] = total(dgy).reshape(d)
        emit(2, dg_ref, dgout_ref)

    if fast:
        es = []
        for h in BOTH:
            he[h].finish()
            es.append(remote(fx.at[h, c], fx.at[h, c], sib_s.at[1, h, 0], sib_r.at[1, h, 0], sib))
            cp = pltpu.make_async_copy(fx.at[h, c], dxall_ref.at[0, c, :, :, pl.ds(h * dh, dh)], osem.at[1, h, 0])
            cp.start()
            outs.append(cp)
        finish_n()
        def whole(h, cc, i):
            cp = pltpu.make_async_copy(gn.at[h, cc], nall_ref.at[cc, :, :, :, pl.ds(h * dh, dh)], osem.at[0, h, i])
            cp.start()
            outs.append(cp)

        for h in BOTH:
            whole(h, c, 0)
        for h in BOTH:
            n2[h].drain(n)
        for h in BOTH:
            whole(h, 1 - c, 1)
        for h in BOTH:
            es[h].wait_recv()
            cp = pltpu.make_async_copy(fx.at[h, 1 - c], dxall_ref.at[0, 1 - c, :, :, pl.ds(h * dh, dh)],
                                       osem.at[1, h, 1])
            cp.start()
            outs.append(cp)
    else:
        finish_n()
        for h in BOTH:
            n2[h].drain(4)
        for h in BOTH:
            e2[h].drain(1)
        for h in BOTH:
            e2[h].finish()
        for i in (2, 1):
            for h in BOTH:
                e2[h].drain(i)
    for cp in sends:
        cp.wait_send()
    for cp in outs:
        cp.wait()


def load_kernel(dims, ids_ref, most_ref):
    k, tl, n = dims["k"], dims["tl"], dims["n"]
    t = ids_ref.shape[1]
    rows = dims["rt"] * 16
    ids = ids_ref[...]
    idt = jnp.transpose(jnp.concatenate([ids, jnp.zeros((8 - k, t), jnp.int32)], axis=0))
    keys = []
    for axis in BOTH:
        tok = lax.broadcasted_iota(jnp.int32, ids.shape, 1) // tl
        tokt = lax.broadcasted_iota(jnp.int32, (t, 1), 0) // tl
        at = [(v // 2 % n if axis else v // (2 * n)) * 2 + v % 2 for v in (tok, tokt)]
        row = at[0] * (n * n) + ids // rows
        row = jnp.concatenate([row[m:m + 1] for m in range(k)], axis=1)
        col = jnp.concatenate([at[1] * (n * n) + idt[:, m:m + 1] // rows for m in range(k)], axis=0)
        keys.append(jnp.max(jnp.sum((row == col).astype(F32), axis=1, keepdims=True)))
    most_ref[0] = jnp.maximum(*keys).astype(jnp.int32)


def tail_kernel(dims, tab_ref, n_ref, dx_ref, w_ref, du_ref, x_ref, dg_ref,
                u_ref, de_ref, dw_ref, xo_ref, dgo_ref, dxb, dxf, dup, uacc, dsem):
    k, tl, side = dims["k"], dims["tl"], dims["n"]
    tb = k * tl
    rt = dims["rt"]
    j = pl.program_id(0)

    nd = 2 * side * tb
    d = dxf.shape[1]
    dh = d // 2

    @pl.when(j == 0)
    def _():
        pltpu.make_async_copy(dx_ref.at[pl.ds(0, nd)], dxb.at[pl.ds(0, nd)], dsem.at[0]).start()

    @pl.when(j == 1)
    def _():
        few = pltpu.make_async_copy(dx_ref.at[pl.ds(0, nd)], dxb.at[pl.ds(0, nd)], dsem.at[0])
        few.wait()
        dxf[pl.ds(0, nd), :] = dxb[pl.ds(0, nd), :].astype(F32)

        @pl.when(tab_ref[4, 0] == 1)
        def _():
            rest = pl.ds(nd, dxf.shape[0] - nd)
            more = pltpu.make_async_copy(dx_ref.at[rest], dxb.at[rest], dsem.at[1])
            more.start()
            more.wait()
            dxf[rest, :] = dxb[rest, :].astype(F32)

    @pl.when(j > 0)
    def _():
        de_ref[...] = jnp.zeros_like(de_ref)

        @pl.loop(tab_ref[3, j - 1], tab_ref[3, j])
        def _(i):
            row = pl.ds(tab_ref[0, i] - (j - 1) * rt, 1)
            for h in BOTH:
                cols = pl.ds(h * dh, dh)
                de_ref[row, cols] = de_ref[row, cols] + dxf[pl.ds(tab_ref[1 + h, i], 1), cols]

    @pl.when(j == 0)
    def _():
        duf = [du_ref[m].astype(F32) for m in range(k)]
        for cc in BOTH:
            for b in range(side * side):
                r = b * 2 + cc
                blk = jnp.concatenate([v[r * tl:(r + 1) * tl] for v in duf], axis=0)
                dup[pl.ds((cc * side * side + b) * tb, tb), :] = blk.astype(BF16)
        uacc[...] = jnp.zeros_like(uacc)
        xo_ref[...] = x_ref[...]
        dgo_ref[...] = dg_ref[...]

    @pl.when(j < dims["nw"])
    def _():
        nv = n_ref[...]
        dw_ref[...] = lax.dot_general(nv, dup[...], (((0,), (0,)), ((), ())), preferred_element_type=F32)
        uacc[...] += jnp.dot(nv, w_ref[...], preferred_element_type=F32)

    @pl.when(j == pl.num_programs(0) - 1)
    def _():
        for m in range(k):
            parts = []
            for b in range(side * side):
                for cc in BOTH:
                    row = (cc * side * side + b) * tb + m * tl
                    parts.append(uacc[pl.ds(row, tl), :])
            u_ref[m] = jnp.concatenate(parts, axis=0).astype(BF16)


def solution(mesh):
    groups = mesh.shape["tp"]
    side = math.isqrt(groups // 2)

    def local(ids, emb, g, w, du, dres):
        k, t = ids.shape
        vl, d = emb.shape
        f = w.shape[1]
        tl = t // groups
        tb = k * tl
        n = side
        dh, dq = d // 2, d // 4
        cw = 256 if dh % 256 == 0 else 128
        rt = vl // 8
        wc = d // 7 if d % 896 == 0 else d // 4
        nw = d // wc
        dims = dict(k=k, tl=tl, d=d, n=n, cw=cw, rt=rt, nw=nw, cb=dq)
        hbm = pl.BlockSpec(memory_space=pl.ANY)
        vm = pl.BlockSpec(memory_space=pltpu.VMEM)
        gshape = (2, 2, n, n, tb, dh)
        oshape = (2, n, n, tb, d)
        comm = lambda cid, fast: pl.pallas_call(
            functools.partial(comm_kernel, dict(dims, fast=fast)),
            out_shape=[
                jax.ShapeDtypeStruct((k, tl, d), BF16),
                jax.ShapeDtypeStruct(oshape, BF16),
                jax.ShapeDtypeStruct(oshape, BF16),
                jax.ShapeDtypeStruct((d,), F32),
                jax.ShapeDtypeStruct((8, k * t), jnp.int32),
            ],
            in_specs=[vm, hbm, vm, vm, vm, vm],
            out_specs=[hbm] * 5,
            scratch_shapes=[
                VMEM((2, vl, dh), BF16), DMA((2,)),
                VMEM((k * t, vl), BF16),
                VMEM((2, 2, n, n * tb, dh), BF16), VMEM((2, n, n * tb, dh), BF16),
                VMEM((2, n, n * tb, dh), F32), VMEM((2, 3, 2, n * tb, dq), F32),
                VMEM((2, n, tb, dh), F32), VMEM((2, 3, 2, tb, dq), F32),
                VMEM((2, 2, n, n * tb, dh), BF16), VMEM((2, n, n * tb, dh), BF16),
                VMEM((2, 3, 2, n * tb, dq), BF16),
                VMEM((2, n, tb, dh), BF16), VMEM((2, 3, 2, tb, dq), BF16),
                VMEM((2, 2, tb, dh), F32), VMEM(gshape, BF16), VMEM(gshape, BF16),
                VMEM((1, d), F32), VMEM((1, d), F32), VMEM((n, 1, d), F32), VMEM((n, 1, d), F32),
                *[DMA((2, 2))] * 2,
                *[DMA((2, 11, 2) if fast else (2, 2, 2, 3, 2))] * 2,
                *[DMA((3 if fast else 4, 2, 3, 2))] * 2,
                *[DMA((2, 2, n))] * 2,
                *[DMA((7,))] * 2, DMA((2, 2, 2) if fast else (2, 2, 2, n)),
                VMEM((2, 2, n, tb, dh), BF16), VMEM((2, n, tb, dh), BF16), VMEM((2, n, tb, dh), BF16),
                VMEM((2, n, tb, dh), BF16), VMEM((2, 2, n, tb, dh), BF16),
                *[DMA((2, 2, 3))] * 2,
                VMEM((k, tl, d), BF16), VMEM((d,), F32), VMEM((8, k * t), jnp.int32), DMA((3,)),
            ],
            compiler_params=pltpu.CompilerParams(collective_id=cid, has_side_effects=True,
                                                 vmem_limit_bytes=62 * 1024 * 1024),
        )
        most = pl.pallas_call(
            functools.partial(load_kernel, dims),
            out_shape=jax.ShapeDtypeStruct((1,), jnp.int32),
            in_specs=[vm],
            out_specs=pl.BlockSpec(memory_space=pltpu.SMEM),
        )(ids)[0]
        xo, nall, dxall, dg, tab = lax.cond(most <= tb, comm(0, True), comm(1, False), ids, emb, g, w, du, dres)
        u, de, dw, xo, dg = pl.pallas_call(
            functools.partial(tail_kernel, dims),
            grid=(vl // rt + 1,),
            out_shape=[
                jax.ShapeDtypeStruct((k, t, f), BF16),
                jax.ShapeDtypeStruct((vl, d), F32),
                jax.ShapeDtypeStruct((d, f), F32),
                jax.ShapeDtypeStruct((k, tl, d), BF16),
                jax.ShapeDtypeStruct((d,), F32),
            ],
            in_specs=[
                pl.BlockSpec(memory_space=pltpu.SMEM),
                pl.BlockSpec((k * t, wc), lambda j: (0, jnp.minimum(j, nw - 1))),
                hbm,
                pl.BlockSpec((wc, f), lambda j: (jnp.minimum(j, nw - 1), 0)),
                pl.BlockSpec((k, t, f), lambda j: (0, 0, 0)),
                pl.BlockSpec((k, tl, d), lambda j: (0, 0, 0)),
                pl.BlockSpec((d,), lambda j: (0,)),
            ],
            out_specs=[
                pl.BlockSpec((k, t, f), lambda j: (0, 0, 0)),
                pl.BlockSpec((rt, d), lambda j: (jnp.maximum(j - 1, 0), 0)),
                pl.BlockSpec((wc, f), lambda j: (jnp.minimum(j, nw - 1), 0)),
                pl.BlockSpec((k, tl, d), lambda j: (0, 0, 0)),
                pl.BlockSpec((d,), lambda j: (0,)),
            ],
            scratch_shapes=[VMEM((k * t, d), BF16), VMEM((k * t, d), F32), VMEM((k * t, f), BF16),
                            VMEM((k * t, f), F32), DMA((2,))],
            compiler_params=pltpu.CompilerParams(vmem_limit_bytes=62 * 1024 * 1024),
        )(tab, nall.reshape(k * t, d), dxall.reshape(k * t, d), w, du, xo, dg)
        return u, xo, de, dw, dg

    return jax.shard_map(
        local,
        mesh=mesh,
        in_specs=(P("dp", None), P("tp", None), P(None), P(None, "tp"), P("dp", None, "tp"), P("dp", "tp", None)),
        out_specs=(P("dp", None, "tp"), P("dp", "tp", None), P(("dp", "tp"), None), P(None, ("dp", "tp")), P("dp")),
        check_vma=False,
    )
```

```python
import functools
import math

import jax
import jax.numpy as jnp
from jax import lax
from jax.experimental import pallas as pl
from jax.experimental.pallas import tpu as pltpu
from jax.sharding import PartitionSpec as P

EPS = 1e-6
F32 = jnp.float32
BF16 = jnp.bfloat16
VMEM = pltpu.VMEM
DMA = pltpu.SemaphoreType.DMA
BOTH = range(2)
WAYS = (1, -1)
SHIFTS = (2, 1, -1)
RING = {(0, 0): 0, (0, 1): 5, (1, 1): 8}


def comm_kernel(dims, ids_ref, emb_ref, g_ref, w_ref, du_ref, dres_ref,
                xout_ref, nall_ref, dxall_ref, dgout_ref, tabout_ref,
                ebuf, esem, oh, pdn, rpdn, s1, r1, t1, r2, xp, rxp, rx1, tx, rx2,
                own, gn, gd, dgp, dgs, dgx, dgy,
                pair_s, pair_r, rs_s, rs_r, ag_s, ag_r, sib_s, sib_r, dg_s, dg_r, osem,
                xc, rxc, rq, cc_e, fx, hop_s, hop_r, x_ref, dg_ref, tab_ref, small_sem):
    k, tl, d, n, fast = dims["k"], dims["tl"], dims["d"], dims["n"], dims["fast"]
    dh, dq, cw = d // 2, d // 4, dims["cw"]
    nch = dh // cw
    cb = dims["cb"]
    tb = k * tl
    t = du_ref.shape[1]
    vl = emb_ref.shape[0]
    me = lax.axis_index("tp")
    c = lax.rem(me, 2)
    x = lax.rem(me // 2, n)
    y = me // (2 * n)

    def dev(yy, xx, cc):
        return {"tp": (yy * n + xx) * 2 + cc}

    def add(v, s):
        return lax.rem(v + s + n, n)

    coord = {"x": x, "y": y}

    def peer(axis, s):
        return dev(y, add(x, s), c) if axis == "x" else dev(add(y, s), x, c)

    gall = g_ref[...].astype(F32).reshape(1, d)
    sib = dev(y, x, 1 - c)
    sends, outs = [], []

    def emit(i, src, dst):
        cp = pltpu.make_async_copy(src, dst, small_sem.at[i])
        cp.start()
        outs.append(cp)

    def remote(src, dst, ss, rs, to):
        cp = pltpu.make_async_remote_copy(src_ref=src, dst_ref=dst, send_sem=ss, recv_sem=rs,
                                          device_id=to, device_id_type=pl.DeviceIdType.MESH)
        cp.start()
        sends.append(cp)
        return cp

    barrier = pltpu.get_barrier_semaphore()
    greet = [sib] + [peer(a, s) for a in ("x", "y") for s in (1, -1, 2)]
    for to in greet:
        pl.semaphore_signal(barrier, inc=1, device_id=to, device_id_type=pl.DeviceIdType.MESH)

    eload = []
    for h in BOTH:
        cp = pltpu.make_async_copy(emb_ref.at[:, pl.ds(h * dh, dh)], ebuf.at[h], esem.at[h])
        cp.start()
        eload.append(cp)

    def scatter_rows(dst, h, j, val, cw):
        cols = pl.ds(pl.multiple_of(j * cw, cw), cw)
        for cc in BOTH:
            for yy in range(n):
                for xx in range(n):
                    p, q = (xx, yy) if h == 0 else (yy, xx)
                    row = ((yy * n + xx) * 2 + cc) * tl
                    blk = jnp.concatenate([val[m * t + row:m * t + row + tl] for m in range(k)], axis=0)
                    dst[h, cc, p, pl.ds(q * tb, tb), cols] = blk.astype(BF16)

    for h in BOTH:
        @pl.loop(0, dh // cb)
        def _(j):
            wj = w_ref[pl.ds(pl.multiple_of(h * dh + j * cb, cb), cb), :]
            v = lax.dot_general(du_ref[...].reshape(k * t, -1), wj,
                                (((1,), (1,)), ((), ())), preferred_element_type=F32)
            scatter_rows(pdn, h, j, v, cb)

    pl.semaphore_wait(barrier, len(greet))
    pair = [remote(pdn.at[h, 1 - c], rpdn.at[h], pair_s.at[0, h], pair_r.at[0, h], sib) for h in BOTH]

    loc = ids_ref[...] - me * vl
    locp = jnp.concatenate([loc, jnp.zeros((8 - k, t), jnp.int32)], axis=0) if k < 8 else loc
    loct = jnp.transpose(locp)
    if not fast:
        step = 64
        ids = lax.broadcasted_iota(jnp.int32, (step, vl), 1)
        for m in range(k):
            for i in range(t // step):
                rows = pl.ds(m * t + i * step, step)
                oh[rows, :] = (loct[i * step:(i + 1) * step, m:m + 1] == ids).astype(BF16)

    nt = k * t
    keyc = jnp.concatenate([loct[:, m:m + 1] for m in range(k)], axis=0)
    keyr = jnp.concatenate([loc[m:m + 1] for m in range(k)], axis=1)
    posc = lax.broadcasted_iota(jnp.int32, (nt, 1), 0)
    posr = lax.broadcasted_iota(jnp.int32, (1, nt), 1)

    class Facts:
        def __init__(self, key, pos):
            self.loc, self.pos = key, pos
            self.tok = pos % t
            blk = self.tok // tl
            self.c, self.at = blk % 2, {"x": (blk // 2) % n, "y": blk // (2 * n)}
            self.here = (key >= 0) & (key < vl)
            self.chip = (key + me * vl) // (2 * vl)
            self.owner = {"x": self.chip % n, "y": self.chip // n}

        def group(self, axis):
            return (self.at[axis] * 2 + self.c) * (n * n) + self.chip

    fr, fc = Facts(keyr, posr), Facts(keyc, posc)

    def rank_row(axis):
        m = (fc.group(axis) == fr.group(axis)) & (posc < posr)
        return jnp.sum(m.astype(F32), axis=0, keepdims=True).astype(jnp.int32)

    def rank_col(axis):
        m = (fc.group(axis) == fr.group(axis)) & (posr < posc)
        return jnp.sum(m.astype(F32), axis=1, keepdims=True).astype(jnp.int32)

    def pick(want, value):
        m = jnp.where(want, (value + 1).astype(F32), 0.0)
        return jnp.sum(m, axis=1, keepdims=True).astype(jnp.int32) - 1

    def table():
        sortr = jnp.where(fr.here, keyr, vl) * nt + posr
        sortc = jnp.where(fc.here, keyc, vl) * nt + posc
        rank = jnp.sum((sortr < sortc).astype(F32), axis=1, keepdims=True)
        hit = rank == posr.astype(F32)
        if fast:
            places = [(fc.c * n + fc.at["y"]) * tb + rank_col("y"), (fc.c * n + fc.at["x"]) * tb + rank_col("x")]
        else:
            place = ((fc.c * n + fc.at["y"]) * n + fc.at["x"]) * tb + (posc // t) * tl + fc.tok % tl
            places = [place]
        vals = [jnp.sum(jnp.where(hit, v.astype(F32), 0.0), axis=0, keepdims=True).astype(jnp.int32)
                for v in [keyc] + places]
        tab_ref[0:1, :] = vals[0]
        tab_ref[1:2, :] = vals[1]
        tab_ref[2:3, :] = vals[-1]
        below = fc.here & (keyc < posr * dims["rt"])
        tab_ref[3:4, :] = jnp.sum(below.astype(F32), axis=0, keepdims=True).astype(jnp.int32)
        tab_ref[4:, :] = jnp.full((4, nt), not fast, jnp.int32)
        emit(0, tab_ref, tabout_ref)

    if not fast:
        table()

    class Ring:
        def __init__(self, sem, axis, s, r, parts=1):
            self.sem, self.axis, self.s, self.r, self.parts = sem, axis, s, r, parts
            self.p = coord[axis]
            self.pr = s.shape[1] // parts
            self.b = []
            self.far_in = False

        def half(self, sgn):
            return pl.ds(0 if sgn > 0 else dq, dq)

        def rows(self, part):
            return pl.ds(part * self.pr, self.pr)

        def send(self, msg, sgn, block, half, part=None):
            i = 0 if sgn > 0 else 1
            st, h, ph = self.sem
            rows = slice(None) if part is None else self.rows(part)
            sem = (h, RING[st, ph] + msg + (part or 0) * 2, i) if fast else (st, h, ph, msg, i)
            return remote(self.s.at[block, rows, half], self.r.at[msg, i, rows],
                          rs_s.at[sem], rs_r.at[sem], peer(self.axis, sgn))

        def start(self):
            self.far()
            self.near(0)

        def far(self):
            self.a1 = [self.send(0, sg, add(self.p, 2), self.half(sg)) for sg in WAYS]

        def near(self, part):
            self.b += [self.send(1, sg, add(self.p, sg), self.half(-sg), part) for sg in WAYS]

        def mid(self, part=0):
            for i, sg in enumerate(WAYS):
                if not self.far_in:
                    self.a1[i].wait_recv()
                blk, rows, hf = add(self.p, sg), self.rows(part), self.half(sg)
                self.s[blk, rows, hf] = self.s[blk, rows, hf] + self.r[0, i, rows]
                self.b.append(self.send(2, sg, blk, hf, part))
            self.far_in = True

        def finish(self):
            for cp in self.b:
                cp.wait_recv()
            for i, sg in enumerate(WAYS):
                hf = self.half(sg)
                yield hf, self.s[self.p, :, hf] + self.r[2, i] + self.r[1, 1 - i]

    axes = [("x", "y"), ("y", "x")]

    def first(st, h, s, r):
        return Ring((st, h, 0), axes[h][0], s, r.at[h], 2 if fast and st == 0 else 1)

    def second(st, h, t, r):
        return Ring((st, h, 1), axes[h][1], t.at[h], r.at[h])

    d1 = [first(0, h, s1.at[h], r1) for h in BOTH]
    d2 = [second(0, h, t1, r2) for h in BOTH]
    x1 = [first(1, h, xp.at[h, c], rx1) for h in BOTH]
    x2 = [second(1, h, tx, rx2) for h in BOTH]

    def finish1(ring, t, h):
        for hf, v in ring.finish():
            t[h, :, :, hf] = v.reshape(n, tb, dq)

    def emm(h):
        @pl.loop(0, nch)
        def _(j):
            ej = ebuf[h, :, pl.ds(pl.multiple_of(j * cw, cw), cw)]
            v = jnp.dot(oh[...], ej, preferred_element_type=F32)
            scatter_rows(xp, h, j, v, cw)

    def start_d1(h):
        pair[h].wait_recv()
        for p in range(n):
            s1[h, p] = pdn[h, c, p].astype(F32) + rpdn[h, p].astype(F32)
        d1[h].far()
        if not fast:
            d1[h].near(0)

    def send_x(h):
        src, dst = (xc.at[h, 1 - c], rxc.at[h]) if fast else (xp.at[h, 1 - c], rxp.at[h])
        return remote(src, dst, pair_s.at[1, h], pair_r.at[1, h], sib)

    def start_x1(h):
        xpair[h].wait_recv()
        for p in range(n):
            xp[h, c, p] = xp[h, c, p] + rxp[h, p]
        x1[h].start()

    class Hop:
        def __init__(self, sem, axis, src, dst):
            self.sem, self.axis, self.src, self.dst = sem, axis, src, dst
            self.p = coord[axis]

        def start(self):
            self.a = []
            for i, sh in enumerate(SHIFTS):
                sem = (*self.sem, i)
                self.a.append(remote(self.src.at[add(self.p, sh)], self.dst.at[self.p],
                                     hop_s.at[sem], hop_r.at[sem], peer(self.axis, sh)))
            self.dst[self.p] = self.src[self.p]

        def finish(self):
            for cp in self.a:
                cp.wait_recv()

    if fast:
        rank = {a: rank_row(a) for a in ("x", "y")}
        slots = 2 * n * tb
        slotc = lax.broadcasted_iota(jnp.int32, (slots, 1), 0)
        lane = lax.broadcasted_iota(jnp.int32, (slots, vl), 1)
        for h in BOTH:
            a = axes[h][0]
            slot = (fr.c * n + fr.at[a]) * tb + rank[a]
            row = pick((slot == slotc) & fr.here & (rank[a] < tb), keyr)
            oh[pl.ds(h * slots, slots), :] = (row == lane).astype(BF16)

        def pack(h):
            eload[h].wait()

            @pl.loop(0, dh // cb)
            def _(j):
                cols = pl.ds(pl.multiple_of(j * cb, cb), cb)
                v = jnp.dot(oh[pl.ds(h * slots, slots), :], ebuf[h, :, cols], preferred_element_type=F32)
                xc[h, :, :, :, cols] = v.reshape(2, n, tb, cb).astype(BF16)

        def chosen(h, fixed, mine, slot_axis, rank_axis):
            other = "y" if slot_axis == "x" else "x"
            i = lax.broadcasted_iota(jnp.int32, (n * tb, 1), 0)
            q = i // tb
            yy, xx = (mine, q) if fixed == "y" else (q, mine)
            pos = ((i % tb) // tl) * t + ((yy * n + xx) * 2 + c) * tl + i % tl
            slot = fr.owner[slot_axis] * tb + rank[rank_axis]
            val = pick((posr == pos) & (fr.owner[other] == coord[other]) & (rank[rank_axis] < tb), slot)
            return (val == lax.broadcasted_iota(jnp.int32, (n * tb, n * tb), 1)).astype(BF16)

        hx = [Hop((0, h), axes[h][0], xc.at[h, c], rq.at[h]) for h in BOTH]
        he = [Hop((1, h), axes[h][1], cc_e.at[h], fx.at[h, c]) for h in BOTH]
        pack(0)
        xpair = [send_x(0)]
        start_d1(0)
        start_d1(1)
        pack(1)
        xpair.append(send_x(1))
        for h in BOTH:
            xpair[h].wait_recv()
            xc[h, c] = xc[h, c] + rxc[h]
            hx[h].start()
        for h in BOTH:
            d1[h].near(0)
        table()
        unpack = [chosen(h, axes[h][0], coord[axes[h][0]], axes[h][0], axes[h][0]) for h in BOTH]
        repack = [chosen(h, axes[h][1], coord[axes[h][1]], axes[h][1], axes[h][1]) for h in BOTH]
        for h in BOTH:
            d1[h].mid(0)
        for h in BOTH:
            hx[h].finish()
            for q in range(0, dh, dq):
                v = jnp.dot(unpack[h], rq[h, :, :, pl.ds(q, dq)].reshape(n * tb, dq), preferred_element_type=F32)
                tx[h, :, :, pl.ds(q, dq)] = v.reshape(n, tb, dq).astype(BF16)
            x2[h].start()
        for h in BOTH:
            d1[h].mid(1)
        for h in BOTH:
            x2[h].mid()
            d1[h].near(1)
    else:
        start_d1(0)
        start_d1(1)
        xpair = []
        for h in BOTH:
            eload[h].wait()
            emm(h)
            xpair.append(send_x(h))
        start_x1(0)
        for h in BOTH:
            d1[h].mid()
        start_x1(1)
        for h in BOTH:
            x1[h].mid()
        finish1(x1[0], tx, 0)
        x2[0].start()
        finish1(d1[0], t1, 0)
        d2[0].start()
        finish1(x1[1], tx, 1)
        x2[1].start()
        finish1(d1[1], t1, 1)
        d2[1].start()
        for h in BOTH:
            x2[h].mid()
        for h in BOTH:
            d2[h].mid()

    class Gather:
        def __init__(self, sem, axis, get, put=None):
            self.sem, self.axis, self.get, self.put = sem, axis, get, put
            self.p = coord[axis]
            self.sibs, self.a = [], []

        def send(self, msg, sgn, block, half):
            i = 0 if sgn > 0 else 1
            st, h, ph = self.sem
            ref = self.get(c, block, half)
            sem = (st * 2 + ph, h, msg, i)
            return remote(ref, ref, ag_s.at[sem], ag_r.at[sem], peer(self.axis, sgn))

        def have(self, s):
            if self.put is None:
                return
            st, h, _ = self.sem
            i = s % n
            ref = self.get(c, add(self.p, s), pl.ds(0, dh))
            self.sibs.append((s, remote(ref, ref, sib_s.at[st, h, i], sib_r.at[st, h, i], sib)))
            if st or not fast:
                self.out(c, s, 0)

        def out(self, cc, s, side):
            st, h, _ = self.sem
            block = add(self.p, s)
            cp = pltpu.make_async_copy(self.get(cc, block, pl.ds(0, dh)), self.put(cc, block),
                                       osem.at[st, h, side, s % n])
            cp.start()
            outs.append(cp)

        def open(self, part):
            self.a += [self.send(part * 2, sg, self.p, pl.ds(part * dq, dq)) for sg in WAYS]

        def start(self):
            self.open(0)
            self.open(1)
            self.have(0)

        def mid(self):
            self.b = []
            for cp in self.a:
                cp.wait_recv()
            for sg in WAYS:
                self.b.append(self.send(1, sg, add(self.p, -sg), pl.ds(0 if sg > 0 else dq, dq)))
            for sg in WAYS:
                self.have(-sg)

        def finish(self):
            for cp in self.b:
                cp.wait_recv()
            self.have(2)

        def drain(self, count):
            for s, cp in self.sibs[:count]:
                cp.wait_recv()
                if not fast:
                    self.out(1 - c, s, 1)
            self.sibs = self.sibs[count:]

    def gathers(st, g, out):
        ph1, ph2 = [], []
        c0, c1 = pl.ds(0, dh), pl.ds(dh, dh)
        ph1.append(Gather((st, 0, 0), "x", lambda cc, i, hf: g.at[0, cc, y, i, :, hf]))
        ph2.append(Gather((st, 0, 1), "y", lambda cc, i, hf: g.at[0, cc, i, :, :, hf],
                          lambda cc, i: out.at[cc, i, :, :, c0]))
        ph1.append(Gather((st, 1, 0), "y", lambda cc, i, hf: g.at[1, cc, i, x, :, hf]))
        ph2.append(Gather((st, 1, 1), "x", lambda cc, i, hf: g.at[1, cc, :, i, :, hf],
                          lambda cc, i: out.at[cc, :, i, :, c1]))
        return ph1, ph2

    n1, n2 = gathers(0, gn, nall_ref)
    e1, e2 = gathers(1, gd, dxall_ref)

    for h in BOTH:
        for hf, v in x2[h].finish():
            own[0, h, :, hf] = v.astype(F32)
    ss = jnp.zeros((tb, 1), F32)
    for h in BOTH:
        v = own[0, h]
        ss = ss + jnp.sum(v * v, axis=-1, keepdims=True)
    rs = lax.rsqrt(ss / d + EPS)
    for h in BOTH:
        gf = gall[:, h * dh:(h + 1) * dh]
        gn[h, c, y, x] = (own[0, h] * rs * gf).astype(BF16)
        n1[h].start()
    for h in BOTH:
        v = own[0, h]
        for m in range(k):
            x_ref[m, :, pl.ds(h * dh, dh)] = v[m * tl:(m + 1) * tl].astype(BF16)
    emit(1, x_ref, xout_ref)

    if fast:
        for h in BOTH:
            finish1(d1[h], t1, h)
            d2[h].start()
        for h in BOTH:
            n1[h].mid()
        for h in BOTH:
            d2[h].mid()
        for h in BOTH:
            n1[h].finish()

    for h in BOTH:
        for hf, v in d2[h].finish():
            own[1, h, :, hf] = v
    dot = jnp.zeros((tb, 1), F32)
    for h in BOTH:
        gf = gall[:, h * dh:(h + 1) * dh]
        nh = own[0, h] * rs
        dot = dot + jnp.sum(nh * (gf * own[1, h]), axis=-1, keepdims=True)
    dot = dot / d
    for h in BOTH:
        gf = gall[:, h * dh:(h + 1) * dh]
        nh = own[0, h] * rs
        dxn = rs * (gf * own[1, h] - nh * dot)
        dr = jnp.concatenate([dres_ref[m, :, pl.ds(h * dh, dh)].astype(F32) for m in range(k)], axis=0)
        gd[h, c, y, x] = (dr + dxn).astype(BF16)
        e1[h].start()
    for h in BOTH:
        dgp[:, pl.ds(h * dh, dh)] = jnp.sum(own[1, h] * (own[0, h] * rs), axis=0, keepdims=True)
    if fast:
        for h in BOTH:
            n2[h].open(0)
            n2[h].open(1)
            n2[h].have(0)
    dgpair = remote(dgp, dgs, dg_s.at[0], dg_r.at[0], sib)

    if not fast:
        for h in BOTH:
            n1[h].mid()
    for h in BOTH:
        e1[h].mid()

    def spread(buf, axis, base):
        return [remote(buf.at[coord[axis]], buf.at[coord[axis]], dg_s.at[base + i], dg_r.at[base + i],
                       peer(axis, s)) for i, s in enumerate((1, -1, 2))]

    def total(buf):
        v = buf[0]
        for i in range(1, n):
            v = v + buf[i]
        return v

    if fast:
        for h in BOTH:
            n2[h].mid()
    dgpair.wait_recv()
    dgx[x] = dgp[...] + dgs[...]
    sx = spread(dgx, "x", 1)
    if not fast:
        for h in BOTH:
            n1[h].finish()
            n2[h].start()
    for h in BOTH:
        e1[h].finish()
        if not fast:
            e2[h].start()
            continue
        for q in range(0, dh, dq):
            cols = pl.ds(q, dq)
            blk = gd[0, c, y, :, :, cols] if h == 0 else gd[1, c, :, x, :, cols]
            v = lax.dot_general(repack[h], blk.reshape(n * tb, dq), (((0,), (0,)), ((), ())),
                                preferred_element_type=F32)
            cc_e[h, :, :, cols] = v.reshape(n, tb, dq).astype(BF16)
        he[h].start()
    for cp in sx:
        cp.wait_recv()
    dgy[y] = total(dgx)
    sy = spread(dgy, "y", 4)
    if not fast:
        for h in BOTH:
            n2[h].mid()
    if not fast:
        for h in BOTH:
            e2[h].mid()

    def finish_n():
        for h in BOTH:
            n2[h].finish()
        for cp in sy:
            cp.wait_recv()
        dg_ref[...] = total(dgy).reshape(d)
        emit(2, dg_ref, dgout_ref)

    if fast:
        es = []
        for h in BOTH:
            he[h].finish()
            es.append(remote(fx.at[h, c], fx.at[h, c], sib_s.at[1, h, 0], sib_r.at[1, h, 0], sib))
            cp = pltpu.make_async_copy(fx.at[h, c], dxall_ref.at[0, c, :, :, pl.ds(h * dh, dh)], osem.at[1, h, 0])
            cp.start()
            outs.append(cp)
        finish_n()
        def whole(h, cc, i):
            cp = pltpu.make_async_copy(gn.at[h, cc], nall_ref.at[cc, :, :, :, pl.ds(h * dh, dh)], osem.at[0, h, i])
            cp.start()
            outs.append(cp)

        for h in BOTH:
            whole(h, c, 0)
        for h in BOTH:
            n2[h].drain(n)
        for h in BOTH:
            whole(h, 1 - c, 1)
        for h in BOTH:
            es[h].wait_recv()
            cp = pltpu.make_async_copy(fx.at[h, 1 - c], dxall_ref.at[0, 1 - c, :, :, pl.ds(h * dh, dh)],
                                       osem.at[1, h, 1])
            cp.start()
            outs.append(cp)
    else:
        finish_n()
        for h in BOTH:
            n2[h].drain(4)
        for h in BOTH:
            e2[h].drain(1)
        for h in BOTH:
            e2[h].finish()
        for i in (2, 1):
            for h in BOTH:
                e2[h].drain(i)
    for cp in sends:
        cp.wait_send()
    for cp in outs:
        cp.wait()


def load_kernel(dims, ids_ref, most_ref):
    k, tl, n = dims["k"], dims["tl"], dims["n"]
    t = ids_ref.shape[1]
    rows = dims["rt"] * 16
    ids = ids_ref[...]
    idt = jnp.transpose(jnp.concatenate([ids, jnp.zeros((8 - k, t), jnp.int32)], axis=0))
    keys = []
    for axis in BOTH:
        tok = lax.broadcasted_iota(jnp.int32, ids.shape, 1) // tl
        tokt = lax.broadcasted_iota(jnp.int32, (t, 1), 0) // tl
        at = [(v // 2 % n if axis else v // (2 * n)) * 2 + v % 2 for v in (tok, tokt)]
        row = at[0] * (n * n) + ids // rows
        row = jnp.concatenate([row[m:m + 1] for m in range(k)], axis=1)
        col = jnp.concatenate([at[1] * (n * n) + idt[:, m:m + 1] // rows for m in range(k)], axis=0)
        keys.append(jnp.max(jnp.sum((row == col).astype(F32), axis=1, keepdims=True)))
    most_ref[0] = jnp.maximum(*keys).astype(jnp.int32)


def tail_kernel(dims, tab_ref, n_ref, dx_ref, w_ref, du_ref, x_ref, dg_ref,
                u_ref, de_ref, dw_ref, xo_ref, dgo_ref, dxb, dxf, dup, uacc, dsem):
    k, tl, side = dims["k"], dims["tl"], dims["n"]
    tb = k * tl
    rt = dims["rt"]
    j = pl.program_id(0)

    nd = 2 * side * tb
    d = dxf.shape[1]
    dh = d // 2

    @pl.when(j == 0)
    def _():
        pltpu.make_async_copy(dx_ref.at[pl.ds(0, nd)], dxb.at[pl.ds(0, nd)], dsem.at[0]).start()

    @pl.when(j == 1)
    def _():
        few = pltpu.make_async_copy(dx_ref.at[pl.ds(0, nd)], dxb.at[pl.ds(0, nd)], dsem.at[0])
        few.wait()
        dxf[pl.ds(0, nd), :] = dxb[pl.ds(0, nd), :].astype(F32)

        @pl.when(tab_ref[4, 0] == 1)
        def _():
            rest = pl.ds(nd, dxf.shape[0] - nd)
            more = pltpu.make_async_copy(dx_ref.at[rest], dxb.at[rest], dsem.at[1])
            more.start()
            more.wait()
            dxf[rest, :] = dxb[rest, :].astype(F32)

    @pl.when(j > 0)
    def _():
        de_ref[...] = jnp.zeros_like(de_ref)

        @pl.loop(tab_ref[3, j - 1], tab_ref[3, j])
        def _(i):
            row = pl.ds(tab_ref[0, i] - (j - 1) * rt, 1)
            for h in BOTH:
                cols = pl.ds(h * dh, dh)
                de_ref[row, cols] = de_ref[row, cols] + dxf[pl.ds(tab_ref[1 + h, i], 1), cols]

    @pl.when(j == 0)
    def _():
        duf = [du_ref[m].astype(F32) for m in range(k)]
        for cc in BOTH:
            for b in range(side * side):
                r = b * 2 + cc
                blk = jnp.concatenate([v[r * tl:(r + 1) * tl] for v in duf], axis=0)
                dup[pl.ds((cc * side * side + b) * tb, tb), :] = blk.astype(BF16)
        uacc[...] = jnp.zeros_like(uacc)
        xo_ref[...] = x_ref[...]
        dgo_ref[...] = dg_ref[...]

    @pl.when(j < dims["nw"])
    def _():
        nv = n_ref[...]
        dw_ref[...] = lax.dot_general(nv, dup[...], (((0,), (0,)), ((), ())), preferred_element_type=F32)
        uacc[...] += jnp.dot(nv, w_ref[...], preferred_element_type=F32)

    @pl.when(j == pl.num_programs(0) - 1)
    def _():
        for m in range(k):
            parts = []
            for b in range(side * side):
                for cc in BOTH:
                    row = (cc * side * side + b) * tb + m * tl
                    parts.append(uacc[pl.ds(row, tl), :])
            u_ref[m] = jnp.concatenate(parts, axis=0).astype(BF16)


def solution(mesh):
    groups = mesh.shape["tp"]
    side = math.isqrt(groups // 2)

    def local(ids, emb, g, w, du, dres):
        k, t = ids.shape
        vl, d = emb.shape
        f = w.shape[1]
        tl = t // groups
        tb = k * tl
        n = side
        dh, dq = d // 2, d // 4
        cw = 256 if dh % 256 == 0 else 128
        rt = vl // 8
        wc = d // 7 if d % 896 == 0 else d // 4
        nw = d // wc
        dims = dict(k=k, tl=tl, d=d, n=n, cw=cw, rt=rt, nw=nw, cb=dq)
        hbm = pl.BlockSpec(memory_space=pl.ANY)
        vm = pl.BlockSpec(memory_space=pltpu.VMEM)
        gshape = (2, 2, n, n, tb, dh)
        oshape = (2, n, n, tb, d)
        comm = lambda cid, fast: pl.pallas_call(
            functools.partial(comm_kernel, dict(dims, fast=fast)),
            out_shape=[
                jax.ShapeDtypeStruct((k, tl, d), BF16),
                jax.ShapeDtypeStruct(oshape, BF16),
                jax.ShapeDtypeStruct(oshape, BF16),
                jax.ShapeDtypeStruct((d,), F32),
                jax.ShapeDtypeStruct((8, k * t), jnp.int32),
            ],
            in_specs=[vm, hbm, vm, vm, vm, vm],
            out_specs=[hbm] * 5,
            scratch_shapes=[
                VMEM((2, vl, dh), BF16), DMA((2,)),
                VMEM((k * t, vl), BF16),
                VMEM((2, 2, n, n * tb, dh), BF16), VMEM((2, n, n * tb, dh), BF16),
                VMEM((2, n, n * tb, dh), F32), VMEM((2, 3, 2, n * tb, dq), F32),
                VMEM((2, n, tb, dh), F32), VMEM((2, 3, 2, tb, dq), F32),
                VMEM((2, 2, n, n * tb, dh), BF16), VMEM((2, n, n * tb, dh), BF16),
                VMEM((2, 3, 2, n * tb, dq), BF16),
                VMEM((2, n, tb, dh), BF16), VMEM((2, 3, 2, tb, dq), BF16),
                VMEM((2, 2, tb, dh), F32), VMEM(gshape, BF16), VMEM(gshape, BF16),
                VMEM((1, d), F32), VMEM((1, d), F32), VMEM((n, 1, d), F32), VMEM((n, 1, d), F32),
                *[DMA((2, 2))] * 2,
                *[DMA((2, 11, 2) if fast else (2, 2, 2, 3, 2))] * 2,
                *[DMA((3 if fast else 4, 2, 3, 2))] * 2,
                *[DMA((2, 2, n))] * 2,
                *[DMA((7,))] * 2, DMA((2, 2, 2) if fast else (2, 2, 2, n)),
                VMEM((2, 2, n, tb, dh), BF16), VMEM((2, n, tb, dh), BF16), VMEM((2, n, tb, dh), BF16),
                VMEM((2, n, tb, dh), BF16), VMEM((2, 2, n, tb, dh), BF16),
                *[DMA((2, 2, 3))] * 2,
                VMEM((k, tl, d), BF16), VMEM((d,), F32), VMEM((8, k * t), jnp.int32), DMA((3,)),
            ],
            compiler_params=pltpu.CompilerParams(collective_id=cid, has_side_effects=True,
                                                 vmem_limit_bytes=62 * 1024 * 1024),
        )
        most = pl.pallas_call(
            functools.partial(load_kernel, dims),
            out_shape=jax.ShapeDtypeStruct((1,), jnp.int32),
            in_specs=[vm],
            out_specs=pl.BlockSpec(memory_space=pltpu.SMEM),
        )(ids)[0]
        xo, nall, dxall, dg, tab = lax.cond(most <= tb, comm(0, True), comm(1, False), ids, emb, g, w, du, dres)
        u, de, dw, xo, dg = pl.pallas_call(
            functools.partial(tail_kernel, dims),
            grid=(vl // rt + 1,),
            out_shape=[
                jax.ShapeDtypeStruct((k, t, f), BF16),
                jax.ShapeDtypeStruct((vl, d), F32),
                jax.ShapeDtypeStruct((d, f), F32),
                jax.ShapeDtypeStruct((k, tl, d), BF16),
                jax.ShapeDtypeStruct((d,), F32),
            ],
            in_specs=[
                pl.BlockSpec(memory_space=pltpu.SMEM),
                pl.BlockSpec((k * t, wc), lambda j: (0, jnp.minimum(j, nw - 1))),
                hbm,
                pl.BlockSpec((wc, f), lambda j: (jnp.minimum(j, nw - 1), 0)),
                pl.BlockSpec((k, t, f), lambda j: (0, 0, 0)),
                pl.BlockSpec((k, tl, d), lambda j: (0, 0, 0)),
                pl.BlockSpec((d,), lambda j: (0,)),
            ],
            out_specs=[
                pl.BlockSpec((k, t, f), lambda j: (0, 0, 0)),
                pl.BlockSpec((rt, d), lambda j: (jnp.maximum(j - 1, 0), 0)),
                pl.BlockSpec((wc, f), lambda j: (jnp.minimum(j, nw - 1), 0)),
                pl.BlockSpec((k, tl, d), lambda j: (0, 0, 0)),
                pl.BlockSpec((d,), lambda j: (0,)),
            ],
            scratch_shapes=[VMEM((k * t, d), BF16), VMEM((k * t, d), F32), VMEM((k * t, f), BF16),
                            VMEM((k * t, f), F32), DMA((2,))],
            compiler_params=pltpu.CompilerParams(vmem_limit_bytes=62 * 1024 * 1024),
        )(tab, nall.reshape(k * t, d), dxall.reshape(k * t, d), w, du, xo, dg)
        return u, xo, de, dw, dg

    return jax.shard_map(
        local,
        mesh=mesh,
        in_specs=(P("dp", None), P("tp", None), P(None), P(None, "tp"), P("dp", None, "tp"), P("dp", "tp", None)),
        out_specs=(P("dp", None, "tp"), P("dp", "tp", None), P(("dp", "tp"), None), P(None, ("dp", "tp")), P("dp")),
        check_vma=False,
    )
```
